128 devices in a mesh: seq: 64 (over z, x, y), batch: 2 (over core).
Axes of the slice: x: 4, y: 4, z: 4, core: 2. Of those that a mesh axis runs over, the one named last changes fastest.
Arguments:
- inputs: bfloat16 [2, 8192, 2048], P('batch', 'seq'), may hold values from -6 to 6
- cotangent: bfloat16 [2, 8192, 1024], P('batch', 'seq'), may hold values from -48 to 48
- w_query: bfloat16 [2048, 128], replicated, may hold values from -0.125 to 0.125
- w_key: bfloat16 [2048, 128], replicated, may hold values from -0.125 to 0.125
- w_value: bfloat16 [2048, 1024], replicated, may hold values from -0.125 to 0.125
Outputs:
- grad_inputs: bfloat16 [2, 8192, 2048], P('batch', 'seq')
- grad_w_query: float32 [2048, 128], P(('seq', 'batch'))
- grad_w_key: float32 [2048, 128], P(('seq', 'batch'))
- grad_w_value: float32 [2048, 1024], P(('seq', 'batch'))
The draws below stay inside these ranges and needn't reach their ends.
All inputs are finite; a program needn't handle non-finite values.
Results may differ from the reference program's by a relative error of at most 0.006.
Values sent between devices are 32-bit elements; how exact they have to be, the bound alone decides.
A program may use at most 128 MiB of HBM per device.

```python
import math
import jax
import jax.numpy as jnp
import numpy as np
from jax import lax

D = 2048
H = 8
DK = 16
DV = 128
F = 153
SEQ_LEN = 8192
SEQS = 2


def shard_levels(stream_key, shape, cuts, least, high):
    gain, own = 1.0, jax.random.fold_in(stream_key, 6)
    for position, parts in cuts:
        draws = jnp.exp(jax.random.uniform(jax.random.fold_in(own, position), (parts,), jnp.float32, least / len(cuts), high / len(cuts)))
        gain = gain * jnp.repeat(draws, shape[position] // parts).reshape([-1 if axis == position else 1 for axis in range(len(shape))])
    return gain


def bell_draw(stream_key, extent, scale, bound, cuts=(), kind=jnp.bfloat16):
    drawn = scale * jax.random.normal(stream_key, extent, jnp.float32)
    if cuts:
        drawn = drawn * shard_levels(stream_key, extent, cuts, -0.22, 0.18)
    return jnp.clip(drawn, -bound, bound).astype(kind)


def setup_inputs(seed: int = 0) -> dict:
    streams_of = jax.random.split(jax.random.key(seed), 6)
    inputs = bell_draw(streams_of[0], (SEQS, SEQ_LEN, D), 1.0, 6.0, ((0, 2), (1, 64)))
    cotangent = bell_draw(streams_of[1], (SEQS, SEQ_LEN, H * DV), 8.0, 48.0, ((0, 2), (1, 64)))
    w_query = bell_draw(streams_of[2], (D, H * DK), D ** -0.5, 0.125)
    w_key = bell_draw(streams_of[3], (D, H * DK), D ** -0.5, 0.125)
    w_value = bell_draw(streams_of[4], (D, H * DV), D ** -0.5, 0.125)
    return dict(inputs=inputs, cotangent=cotangent, w_query=w_query, w_key=w_key, w_value=w_value)


highest = lax.Precision.HIGHEST

def pair_tables(width):
    rows_idx, cols_idx = np.triu_indices(width)
    eye_table = np.eye(width, dtype=np.float32)
    left_pick = jnp.asarray(eye_table[rows_idx])
    right_pick = jnp.asarray(eye_table[cols_idx])
    pair_coef = jnp.asarray(np.where(rows_idx == cols_idx, 1.0 / math.sqrt(2.0), 1.0).astype(np.float32))
    return (left_pick, right_pick, pair_coef)

def features(scaled, tables):
    left_pick, right_pick, pair_coef = tables
    left_val = jnp.einsum('...d,pd->...p', scaled, left_pick, precision=highest)
    right_val = jnp.einsum('...d,pd->...p', scaled, right_pick, precision=highest)
    leading = jnp.ones(scaled.shape[:-1] + (1,), jnp.float32)
    return jnp.concatenate([leading, scaled, left_val * right_val * pair_coef], -1)

def pull_back(scaled, grad_feat, tables):
    left_pick, right_pick, pair_coef = tables
    width = scaled.shape[-1]
    linear_part = grad_feat[..., 1:1 + width]
    pair_grad = grad_feat[..., 1 + width:] * pair_coef
    left_val = jnp.einsum('...d,pd->...p', scaled, left_pick, precision=highest)
    right_val = jnp.einsum('...d,pd->...p', scaled, right_pick, precision=highest)
    result = linear_part + jnp.einsum('...p,pd->...d', pair_grad * right_val, left_pick, precision=highest)
    return result + jnp.einsum('...p,pd->...d', pair_grad * left_val, right_pick, precision=highest)

def reference(inputs, cotangent, w_query, w_key, w_value):
    tables = pair_tables(DK)
    flat = inputs.reshape(SEQS * SEQ_LEN, D)
    query = jnp.dot(flat, w_query, preferred_element_type=jnp.float32).reshape(SEQS, SEQ_LEN, H, DK)
    keys = jnp.dot(flat, w_key, preferred_element_type=jnp.float32).reshape(SEQS, SEQ_LEN, H, DK)
    values = jnp.dot(flat, w_value, preferred_element_type=jnp.float32).astype(jnp.bfloat16).reshape(SEQS, SEQ_LEN, H, DV)
    feat_q = features(query * 0.5, tables).astype(jnp.bfloat16)
    feat_k = features(keys * 0.5, tables).astype(jnp.bfloat16)
    upstream = cotangent.astype(jnp.float32).reshape(SEQS, SEQ_LEN, H, DV)
    block_len = math.gcd(512, SEQ_LEN)
    nblocks = SEQ_LEN // block_len

    def blocked(array):
        return array.reshape((SEQS, nblocks, block_len) + array.shape[2:]).swapaxes(0, 1)

    def unblocked(array):
        return array.swapaxes(0, 1).reshape((SEQS, SEQ_LEN) + array.shape[3:])
    causal = lax.broadcasted_iota(jnp.int32, (block_len, block_len), 0) >= lax.broadcasted_iota(jnp.int32, (block_len, block_len), 1)

    def scores(fq32, fk32):
        attn = jnp.einsum('bthf,bshf->bhts', fq32, fk32, precision=highest)
        return jnp.where(causal, attn, 0.0)

    def grad_scores(grad_numer, grad_denom, val32):
        inner = jnp.einsum('bthe,bshe->bhts', grad_numer, val32, precision=highest)
        inner = inner + jnp.transpose(grad_denom, (0, 2, 1))[:, :, :, None]
        return jnp.where(causal, inner, 0.0)

    def forward_step(carry, pieces):
        state, norm_state = carry
        fq_blk, fk_blk, val_blk, up_blk = pieces
        fq32 = fq_blk.astype(jnp.float32)
        fk32 = fk_blk.astype(jnp.float32)
        val32 = val_blk.astype(jnp.float32)
        attn = scores(fq32, fk32)
        numerator = jnp.einsum('bhts,bshe->bthe', attn, val32, precision=highest)
        numerator = numerator + jnp.einsum('bthf,bhfe->bthe', fq32, state, precision=highest)
        denominator = jnp.transpose(lax.optimization_barrier(jnp.sum(attn, -1)), (0, 2, 1))
        denominator = denominator + jnp.einsum('bthf,bhf->bth', fq32, norm_state, precision=highest)
        output = numerator / denominator[..., None]
        grad_numer = up_blk / denominator[..., None]
        grad_denom = -lax.optimization_barrier(jnp.sum(up_blk * output, -1)) / denominator
        grad_attn = grad_scores(grad_numer, grad_denom, val32)
        grad_fq = jnp.einsum('bhts,bshf->bthf', grad_attn, fk32, precision=highest)
        grad_fq = grad_fq + jnp.einsum('bhfe,bthe->bthf', state, grad_numer, precision=highest)
        grad_fq = grad_fq + norm_state[:, None, :, :] * grad_denom[..., None]
        state = state + jnp.einsum('bshf,bshe->bhfe', fk32, val32, precision=highest)
        norm_state = norm_state + lax.optimization_barrier(jnp.sum(fk32, 1))
        return ((state, norm_state), (grad_numer, grad_denom, grad_fq))
    start_state = (jnp.zeros((SEQS, H, F, DV), jnp.float32), jnp.zeros((SEQS, H, F), jnp.float32))
    _, (grad_numer, grad_denom, grad_fq) = lax.scan(forward_step, start_state, (blocked(feat_q), blocked(feat_k), blocked(values), blocked(upstream)))

    def reverse_step(carry, pieces):
        back_state, back_norm = carry
        fq_blk, fk_blk, val_blk, numer_blk, denom_blk = pieces
        fq32 = fq_blk.astype(jnp.float32)
        fk32 = fk_blk.astype(jnp.float32)
        val32 = val_blk.astype(jnp.float32)
        attn = scores(fq32, fk32)
        grad_attn = grad_scores(numer_blk, denom_blk, val32)
        grad_val = jnp.einsum('bhts,bthe->bshe', attn, numer_blk, precision=highest)
        grad_val = grad_val + jnp.einsum('bshf,bhfe->bshe', fk32, back_state, precision=highest)
        grad_fk = jnp.einsum('bhts,bthf->bshf', grad_attn, fq32, precision=highest)
        grad_fk = grad_fk + jnp.einsum('bshe,bhfe->bshf', val32, back_state, precision=highest)
        grad_fk = grad_fk + back_norm[:, None, :, :]
        back_state = back_state + jnp.einsum('bthf,bthe->bhfe', fq32, numer_blk, precision=highest)
        back_norm = back_norm + jnp.einsum('bthf,bth->bhf', fq32, denom_blk, precision=highest)
        return ((back_state, back_norm), (grad_val, grad_fk))
    _, (grad_val, grad_fk) = lax.scan(reverse_step, start_state, (blocked(feat_q), blocked(feat_k), blocked(values), grad_numer, grad_denom), reverse=True)
    grad_fq = unblocked(grad_fq)
    grad_fk = unblocked(grad_fk)
    grad_val = unblocked(grad_val)
    grad_query = (pull_back(query * 0.5, grad_fq, tables) * 0.5).astype(jnp.bfloat16).reshape(SEQS * SEQ_LEN, H * DK)
    grad_keys = (pull_back(keys * 0.5, grad_fk, tables) * 0.5).astype(jnp.bfloat16).reshape(SEQS * SEQ_LEN, H * DK)
    grad_values = grad_val.astype(jnp.bfloat16).reshape(SEQS * SEQ_LEN, H * DV)
    grad_in = jnp.dot(grad_query, w_query.T, preferred_element_type=jnp.float32)
    grad_in = grad_in + jnp.dot(grad_keys, w_key.T, preferred_element_type=jnp.float32)
    grad_in = grad_in + jnp.dot(grad_values, w_value.T, preferred_element_type=jnp.float32)
    grad_in = grad_in.astype(jnp.bfloat16).reshape(SEQS, SEQ_LEN, D)
    grad_wq = jnp.dot(flat.T, grad_query, preferred_element_type=jnp.float32)
    grad_wk = jnp.dot(flat.T, grad_keys, preferred_element_type=jnp.float32)
    grad_wv = jnp.dot(flat.T, grad_values, preferred_element_type=jnp.float32)
    return (grad_in, grad_wq, grad_wk, grad_wv)
```

```python
import functools
import math

import jax
import jax.numpy as jnp
from jax import lax
from jax.experimental import pallas as pl
from jax.experimental.pallas import tpu as pltpu
from jax.sharding import PartitionSpec as P

H = 8
DK = 16
DV = 128
F = 160
T = 128
N = 64
PART = F // 8
D = 2048
UNITS = 20
MESH = pl.DeviceIdType.MESH
BF = jnp.bfloat16
F32 = jnp.float32
ROOT = 1.0 / math.sqrt(2.0)
HBM = pl.BlockSpec(memory_space=pl.ANY)
VMEM = pl.BlockSpec(memory_space=pltpu.VMEM)


def dot(left, right, dims=(1, 0)):
    return lax.dot_general(left, right, ((dims[:1], dims[1:]), ((), ())), preferred_element_type=F32)


def halves(a):
    high = a.astype(BF)
    return high, (a - high.astype(F32)).astype(BF)


def dot2(pair, right, dims=(1, 0)):
    return dot(pair[0], right, dims) + dot(pair[1], right, dims)


def dot2r(left, pair, dims=(1, 0)):
    return dot(left, pair[0], dims) + dot(left, pair[1], dims)


def dot3(lefts, rights, dims=(1, 0)):
    return (
        dot(lefts[0], rights[0], dims)
        + dot(lefts[0], rights[1], dims)
        + dot(lefts[1], rights[0], dims)
    )


def ahead(a, d):
    return pltpu.roll(a, (8 - d) % 8, 0) if d % 8 else a


def back(a, d):
    return pltpu.roll(a, d, 0) if d % 8 else a


def phi(u):
    row = lax.broadcasted_iota(jnp.int32, (8, T), 0)
    low, high = u[:8], u[8:]
    tiles = []
    for m, fill in ((low, jnp.zeros((8, T), F32)), (high, (row == 4).astype(F32))):
        tiles.append(m * m * ROOT)
        for d in range(1, 4):
            tiles.append(m * ahead(m, d))
        tiles.append(jnp.where(row < 4, m * ahead(m, 4), fill))
    for d in range(8):
        tiles.append(low * ahead(high, d))
    return jnp.concatenate(tiles + [low, high], 0)


def pull(u, grad):
    row = lax.broadcasted_iota(jnp.int32, (8, T), 0)
    low, high = u[:8], u[8:]
    tile = lambda n: grad[8 * n : 8 * n + 8]
    sums = []
    for at, m in ((0, low), (5, high)):
        total = tile(18 + at // 5) + tile(at) * (2.0 * ROOT) * m
        for d in range(1, 5):
            piece = tile(at + d)
            if d == 4:
                piece = jnp.where(row < 4, piece, 0.0)
            total = total + piece * ahead(m, d) + back(piece * m, d)
        sums.append(total)
    for d in range(8):
        piece = tile(10 + d)
        sums[0] = sums[0] + piece * ahead(high, d)
        sums[1] = sums[1] + back(piece * low, d)
    return jnp.concatenate(sums, 0)


def kernel(
    x_hbm, c_hbm, wq_hbm, wk_hbm, wv_hbm, gi_ref, oq_ref, ok_ref, ov_ref,
    x_ref, c_ref, wq_ref, wk_ref, wv_ref,
    uq_ref, uk_ref, fqt, fkt, fqn, fkn, v_ref, ath, atl, ni_ref, rd_ref, gnh, gnl, ga_ref,
    gv_ref, gk_ref, sh_ref, gt_ref,
    s1, s2, s3, s4, t1, t2, t3, t4, nsrc, nrcv, tsrc, trcv,
    xt_ref, xr_ref, xp_ref, gs_ref, gr_ref, gp_ref,
    p_ref, a_ref, b_ref, q_ref, r2_ref, w_ref, r3_ref,
    load, a2s, a2r, lns, lnr, xs, xr, gss, grr, p1s, p1r, p2s, p2r, p3s, p3r,
):
    me = lax.axis_index("seq")
    core = lax.axis_index("batch")
    other = 1 - core
    at = (me // 16, (me // 4) % 4, me % 4)
    weight = (16, 4, 1)
    sends = []

    def along(d, c):
        return (me + (c - at[d]) * weight[d], core)

    def copy_to(src, dst, send, recv, device):
        return pltpu.make_async_remote_copy(
            src_ref=src, dst_ref=dst, send_sem=send, recv_sem=recv,
            device_id=device, device_id_type=MESH,
        )

    def push(src, dst, send, recv, device):
        copy = copy_to(src, dst, send, recv, device)
        copy.start()
        sends.append(copy)
        return copy

    loads = []
    for n, (src, dst) in enumerate(
        ((x_hbm, x_ref), (wk_hbm, wk_ref), (wq_hbm, wq_ref), (wv_hbm, wv_ref), (c_hbm, c_ref))
    ):
        copy = pltpu.make_async_copy(src, dst, load.at[n])
        copy.start()
        loads.append(copy)

    barrier = pltpu.get_barrier_semaphore()

    def greet(k, carry):
        pl.semaphore_signal(barrier, inc=1, device_id=((me + k) % N, core), device_id_type=MESH)
        return carry

    lax.fori_loop(1, N, greet, 0)
    pl.semaphore_signal(barrier, inc=1, device_id=(me, other), device_id_type=MESH)

    def scatter(src, dst, n):
        def step(k, carry):
            peer = (me + k) % N
            copy_to(src.at[peer], dst.at[me], a2s.at[n, peer], a2r.at[n, me], (peer, core)).start()
            return carry

        lax.fori_loop(1, N, step, 0)
        dst[me] = src[me]

    def arrive(dst, n, j):
        @pl.when(j != me)
        def _():
            copy_to(dst.at[j], dst.at[j], a2s.at[n, j], a2r.at[n, j], (j, core)).wait_recv()

    def sent(src, n):
        def step(k, carry):
            peer = (me + k) % N
            copy_to(src.at[peer], src.at[peer], a2s.at[n, peer], a2r.at[n, peer], (peer, core)).wait_send()
            return carry

        lax.fori_loop(1, N, step, 0)

    def scan(src, dst, n, reverse):
        def step(i, run):
            j = N - 1 - i if reverse else i
            arrive(src, n, j)
            dst[j] = run
            return run + src[j]

        lax.fori_loop(0, N, step, jnp.zeros((PART, DV), F32))

    def arrive_all(dst, n):
        def step(j, carry):
            arrive(dst, n, j)
            return carry

        lax.fori_loop(0, N, step, 0)

    def put_state(dst, h, value):
        for j in range(8):
            dst[8 * h + j, :16, :] = value[16 * j : 16 * j + 16]
            dst[8 * h + j, 16:, :] = value[128 + 4 * j : 132 + 4 * j]

    def get_state(src, h):
        tiles = [src[8 * h + j, :16, :] for j in range(8)]
        tiles += [src[8 * h + j, 16:, :] for j in range(8)]
        return jnp.concatenate(tiles, 0)

    def line_send(src, rcv, n, d):
        for k in range(1, 4):
            c = (at[d] + k) % 4
            push(src.at[d], rcv.at[d, at[d]], lns.at[n, d, k], lnr.at[n, d, at[d]], along(d, c))

    def line_sum(src, rcv, n, d, reverse):
        for k in range(1, 4):
            c = (at[d] + k) % 4
            copy_to(src.at[d], rcv.at[d, c], lns.at[n, d, k], lnr.at[n, d, c], along(d, c)).wait_recv()
        rcv[d, at[d]] = src[d]
        total = jnp.zeros((8, 256), F32)
        part = jnp.zeros((8, 256), F32)
        for c in range(4):
            block = rcv[d, c]
            total = total + block
            keep = c > at[d] if reverse else c < at[d]
            part = part + jnp.where(keep, block, 0.0)
        return total, part

    causal = lax.broadcasted_iota(jnp.int32, (T, T), 0) >= lax.broadcasted_iota(jnp.int32, (T, T), 1)
    anti = lax.broadcasted_iota(jnp.int32, (T, T), 0) <= lax.broadcasted_iota(jnp.int32, (T, T), 1)
    lane = lax.broadcasted_iota(jnp.int32, (T, DV), 1)
    ones = jnp.ones((T, DV), BF)
    rows8 = lax.broadcasted_iota(jnp.int32, (8, F), 0)

    loads[0].wait()
    loads[1].wait()
    x = x_ref[...]
    flat = dot(x, wk_ref[...]).T * 0.5
    norm = jnp.zeros((8, F), F32)
    for h in range(H):
        u = flat[DK * h : DK * h + DK]
        uk_ref[h] = u
        f = phi(u)
        ft = f.astype(BF)
        fkt[h] = ft
        fkn[h] = f.T.astype(BF)
        norm = jnp.where(rows8 == h, dot(jnp.ones((8, T), BF), ft, (1, 1)), norm)
    nsrc[2] = jnp.concatenate([norm, jnp.zeros((8, 256 - F), F32)], 1)
    pl.semaphore_wait(barrier, N)
    line_send(nsrc, nrcv, 0, 2)

    loads[3].wait()
    for h in range(H):
        val = dot(x, wv_ref[:, h * DV : (h + 1) * DV]).astype(BF)
        v_ref[h] = val
        put_state(s1, h, dot(fkt[h], val))
    scatter(s1, s2, 0)

    total, prefix = line_sum(nsrc, nrcv, 0, 2, False)
    nsrc[1] = total
    line_send(nsrc, nrcv, 0, 1)

    loads[2].wait()
    flat = dot(x, wq_ref[...]).T * 0.5
    for h in range(H):
        u = flat[DK * h : DK * h + DK]
        uq_ref[h] = u
        f = phi(u)
        fqt[h] = f.astype(BF)
        fqn[h] = f.T.astype(BF)

    total, part = line_sum(nsrc, nrcv, 0, 1, False)
    prefix = prefix + part
    nsrc[0] = total
    line_send(nsrc, nrcv, 0, 0)

    def inside(h):
        attn = halves(jnp.where(causal, dot(fqn[h], fkt[h]), 0.0))
        both = dot2(attn, jnp.concatenate([v_ref[h], ones], 1))
        ni_ref[h] = both[:, :DV]
        rd_ref[h] = both[:, DV:]
        turned = halves(jnp.where(anti, dot(fkn[h], fqt[h]), 0.0))
        ath[h] = turned[0]
        atl[h] = turned[1]

    for h in range(H):
        inside(h)
    total, part = line_sum(nsrc, nrcv, 0, 0, False)
    prefix = prefix + part
    loads[4].wait()

    for h in range(H):
        row = halves(jnp.broadcast_to(prefix[h : h + 1, :F], (DV, F)))
        den = rd_ref[h] + dot2r(fqn[h], row, (1, 1))
        scale = 1.0 / den
        rd_ref[h] = scale
        numer = c_ref[:, h * DV : (h + 1) * DV].astype(F32) * scale
        gn = halves(numer)
        gnh[h] = gn[0]
        gnl[h] = gn[1]
        put_state(t1, h, dot2r(fqt[h], gn))
    scatter(t1, t2, 2)

    for h in range(H):
        gn = (gnh[h], gnl[h])
        gv_ref[h] = dot3((ath[h], atl[h]), gn)
        ga_ref[h] = dot2(gn, v_ref[h], (1, 1))

    scan(s2, s3, 0, False)
    scatter(s3, s4, 1)

    for b in range(D // 128):
        block = x_ref[:, b * 128 : (b + 1) * 128].astype(F32).T
        for i in range(4):
            for half in range(2):
                row = 32 * i + 16 * half
                xt_ref[half, 4 * b + i] = block[row : row + 16]
    swap = push(xt_ref.at[other], xr_ref, xs.at[0], xr.at[0], (me, other))
    xp_ref[:, :T] = xt_ref[core].reshape(D // 2, T).astype(BF)

    scan(t2, t3, 2, True)
    scatter(t3, t4, 3)

    turned = jnp.concatenate([prefix, jnp.zeros((T - 8, 256), F32)], 0).T[:F]
    columns = halves(turned)
    arrive_all(s4, 1)
    down = jnp.zeros((F, DV), F32)
    grads = []
    for h in range(H):
        state = halves(get_state(s4, h))
        gn = (gnh[h], gnl[h])
        num = ni_ref[h] + dot2r(fqn[h], state)
        numer = gn[0].astype(F32) + gn[1].astype(F32)
        denom = -jnp.sum(numer * num, 1, keepdims=True) * rd_ref[h]
        ga = halves(jnp.where(causal, ga_ref[h] + denom, 0.0))
        mine = halves(jnp.where(lane == h, denom, 0.0))
        left = [jnp.concatenate([s, c], 1) for s, c in zip(state, columns)]
        right = [jnp.concatenate([g, m], 1) for g, m in zip(gn, mine)]
        gfq = dot2r(fkt[h], ga, (1, 1)) + dot3(left, right, (1, 1))
        grads.append(pull(uq_ref[h], gfq) * 0.5)
        gk_ref[h] = dot2r(fqt[h], ga)
        down = down + dot2r(fqt[h], mine)
    rows = jnp.concatenate([down, jnp.zeros((256 - F, DV), F32)], 0).T
    tsrc[2] = rows[:8]
    line_send(tsrc, trcv, 1, 2)
    grad_q = jnp.concatenate(grads, 0).T.astype(BF)

    def share(m, value):
        gp_ref[:T, 256 * m : 256 * m + 256] = value
        gs_ref[m] = value.astype(F32)
        return push(gs_ref.at[m], gr_ref.at[m], gss.at[m], grr.at[m], (me, other))

    arrive_all(t4, 3)
    shares = []
    for m in range(4):
        pieces = []
        for h in (2 * m, 2 * m + 1):
            state = halves(get_state(t4, h))
            sh_ref[h] = state[0]
            gt_ref[h] = state[1]
            pieces.append((gv_ref[h] + dot2r(fkn[h], state)).astype(BF))
        shares.append(share(m, jnp.concatenate(pieces, 1)))

    total, suffix = line_sum(tsrc, trcv, 1, 2, True)
    tsrc[1] = total
    line_send(tsrc, trcv, 1, 1)

    swap.wait_recv()
    xp_ref[:, T:] = xr_ref[...].reshape(D // 2, T).astype(BF)

    def multiply(m):
        shares[m].wait_recv()
        gp_ref[T:, 256 * m : 256 * m + 256] = gr_ref[m].astype(BF)
        right = gp_ref[:, 256 * m : 256 * m + 256]
        for z in range(4):
            part = dot(xp_ref[256 * z : 256 * z + 256, :], right)
            for i in range(2):
                block = part[:, i * DV : (i + 1) * DV].reshape(4, 4, 2, 8, DV)
                for r in range(2):
                    p_ref[4 * m + 2 * i + r, z] = block[:, :, r]

    def line_part(u, g, c, half):
        take = pl.ds(2 * half, 2)
        if g == 0:
            return (u, c, take)
        if g == 1:
            return (u, take, c)
        return (u, take, slice(None), c)

    first = {}

    def stage0(u):
        g = u % 3
        i = at[g]
        right, left, far = (i + 1) % 4, (i + 3) % 4, (i + 2) % 4
        keys = (
            (far, 0, right, a_ref.at[u, 0]),
            (far, 1, left, a_ref.at[u, 1]),
            (right, 1, right, b_ref.at[u, 0, pl.ds(2, 2)]),
            (left, 0, left, b_ref.at[u, 1, pl.ds(0, 2)]),
        )
        first[u] = [
            push(p_ref.at[line_part(u, g, c, half)], dst, p1s.at[u, n], p1r.at[u, n], along(g, peer))
            for n, (c, half, peer, dst) in enumerate(keys)
        ]

    def stage1(u):
        g = u % 3
        i = at[g]
        right, left = (i + 1) % 4, (i + 3) % 4
        for n, (peer, half) in enumerate(((right, 0), (left, 1))):
            first[u][n].wait_recv()
            where = line_part(u, g, peer, half)
            p_ref[where] = p_ref[where] + a_ref[u, n]
            dst = b_ref.at[u, n, pl.ds(2 * half, 2)]
            first[u].append(
                push(p_ref.at[where], dst, p1s.at[u, 4 + n], p1r.at[u, 4 + n], along(g, peer))
            )

    order = ((1, 2), (2, 0), (0, 1))

    def stage2(u):
        g = u % 3
        for n in range(2, 6):
            first[u][n].wait_recv()
        for half in range(2):
            mine = p_ref[line_part(u, g, at[g], half)]
            mine = mine + b_ref[u, 0, 2 * half : 2 * half + 2] + b_ref[u, 1, 2 * half : 2 * half + 2]
            for i in range(2):
                if g == 1:
                    q_ref[u, :, 2 * half + i] = mine[i]
                else:
                    q_ref[u, 2 * half + i] = mine[i]
        d = order[g][0]
        first[u] = []
        for k in range(1, 4):
            c = (at[d] + k) % 4
            first[u].append(
                push(q_ref.at[u, c], r2_ref.at[u, at[d]], p2s.at[u, k], p2r.at[u, at[d]], along(d, c))
            )

    def from_line(d, src, dst, send, recv, u):
        for k in range(1, 4):
            c = (at[d] + k) % 4
            copy_to(src.at[u, c], dst.at[u, c], send.at[u, k], recv.at[u, c], along(d, c)).wait_recv()
        total = src[u, at[d]]
        for k in range(1, 4):
            total = total + dst[u, (at[d] + k) % 4]
        return total

    def stage3(u):
        d, e = order[u % 3]
        w_ref[u] = from_line(d, q_ref, r2_ref, p2s, p2r, u)
        for k in range(1, 4):
            c = (at[e] + k) % 4
            push(w_ref.at[u, c], r3_ref.at[u, at[e]], p3s.at[u, k], p3r.at[u, at[e]], along(e, c))

    def stage4(u):
        total = from_line(order[u % 3][1], w_ref, r3_ref, p3s, p3r, u)
        piece, r = u // 2, u % 2
        rows = slice(8 * r, 8 * r + 8)
        if piece < H:
            ov_ref[rows, piece * DV : (piece + 1) * DV] = total
        else:
            (oq_ref if piece == H else ok_ref)[rows, :] = total

    multiply(0)
    for u in range(4):
        stage0(u)
    multiply(1)
    for u in range(4, 8):
        stage0(u)

    total, part = line_sum(tsrc, trcv, 1, 1, True)
    suffix = suffix + part
    tsrc[0] = total
    line_send(tsrc, trcv, 1, 0)

    multiply(2)
    for u in range(8, 12):
        stage0(u)
    multiply(3)
    for u in range(12, 16):
        stage0(u)
    for u in range(6):
        stage1(u)

    total, part = line_sum(tsrc, trcv, 1, 0, True)
    suffix = suffix + part
    turned = jnp.concatenate([suffix, jnp.zeros((T - 8, 256), F32)], 0).T[:F]
    grads = []
    for h in range(H):
        gfk = gk_ref[h] + dot2((sh_ref[h], gt_ref[h]), v_ref[h], (1, 1)) + turned[:, h : h + 1]
        grads.append(pull(uk_ref[h], gfk) * 0.5)
    grad_k = jnp.concatenate(grads, 0).T.astype(BF)
    shares.append(share(4, jnp.concatenate([grad_q, grad_k], 1)))
    for u in range(6, 12):
        stage1(u)
    multiply(4)
    for u in range(16, 20):
        stage0(u)
    for u in range(12, 16):
        stage1(u)

    wide = D // 8

    def inputs(n):
        cut = slice(n * wide, (n + 1) * wide)
        total = dot(gp_ref[:T, : H * DV], wv_ref[cut, :], (1, 1))
        total = total + dot(gp_ref[:T, H * DV : H * DV + 128], wq_ref[cut, :], (1, 1))
        total = total + dot(gp_ref[:T, H * DV + 128 :], wk_ref[cut, :], (1, 1))
        gi_ref[:, cut] = total.astype(BF)

    for n in range(2):
        inputs(n)
    for u in range(8):
        stage2(u)
    for n in range(2, 4):
        inputs(n)
    for u in range(16, 20):
        stage1(u)
    for n in range(4, 6):
        inputs(n)
    for u in range(8, 16):
        stage2(u)
    for u in range(8):
        stage3(u)
    for n in range(6, 8):
        inputs(n)
    for u in range(16, 20):
        stage2(u)
    for u in range(8, 16):
        stage3(u)
    for u in range(8):
        stage4(u)
    for u in range(16, 20):
        stage3(u)
    for u in range(8, 20):
        stage4(u)
    for copy in sends:
        copy.wait_send()
    for n, src in enumerate((s1, s3, t1, t3)):
        sent(src, n)


def body(inputs, cotangent, w_query, w_key, w_value):
    vm = lambda *shape: pltpu.VMEM(shape, F32)
    vb = lambda *shape: pltpu.VMEM(shape, BF)
    sems = lambda *sizes: pltpu.SemaphoreType.DMA(sizes)
    state = lambda: vm(N, PART, DV)
    scratch = [
        vb(T, D), vb(T, H * DV), vb(D, 128), vb(D, 128), vb(D, H * DV),
        vm(H, DK, T), vm(H, DK, T), vb(H, F, T), vb(H, F, T), vb(H, T, F), vb(H, T, F), vb(H, T, DV),
        vb(H, T, T), vb(H, T, T), vm(H, T, DV), vm(H, T, DV), vb(H, T, DV), vb(H, T, DV), vm(H, T, T),
        vm(H, T, DV), vm(H, F, T), vb(H, F, DV), vb(H, F, DV),
        state(), state(), state(), state(), state(), state(), state(), state(),
        vm(3, 8, 256), vm(3, 4, 8, 256), vm(3, 8, 256), vm(3, 4, 8, 256),
        vm(2, N, 16, T), vm(N, 16, T), vb(D // 2, 2 * T), vm(5, T, 256), vm(5, T, 256), vb(2 * T, 1280),
        vm(UNITS, 4, 4, 4, 8, DV), vm(UNITS, 2, 2, 4, 8, DV), vm(UNITS, 2, 4, 4, 8, DV),
        vm(UNITS, 4, 4, 8, DV), vm(UNITS, 4, 4, 8, DV), vm(UNITS, 4, 8, DV), vm(UNITS, 4, 8, DV),
        sems(5), sems(4, N), sems(4, N), sems(2, 3, 4), sems(2, 3, 4), sems(1), sems(1), sems(5), sems(5),
        sems(UNITS, 6), sems(UNITS, 6), sems(UNITS, 4), sems(UNITS, 4), sems(UNITS, 4), sems(UNITS, 4),
    ]
    grad_in, grad_wq, grad_wk, grad_wv = pl.pallas_call(
        kernel,
        out_shape=[
            jax.ShapeDtypeStruct((T, D), BF),
            jax.ShapeDtypeStruct((16, 128), F32),
            jax.ShapeDtypeStruct((16, 128), F32),
            jax.ShapeDtypeStruct((16, H * DV), F32),
        ],
        in_specs=[HBM] * 5,
        out_specs=[VMEM] * 4,
        scratch_shapes=scratch,
        compiler_params=pltpu.CompilerParams(
            collective_id=0, has_side_effects=True, vmem_limit_bytes=60 << 20
        ),
    )(inputs[0], cotangent[0], w_query, w_key, w_value)
    return (grad_in[None], grad_wq, grad_wk, grad_wv)


def solution(mesh):
    in_specs = (P("batch", "seq", None), P("batch", "seq", None), P(), P(), P())
    out_specs = (
        P("batch", "seq", None),
        P(("seq", "batch"), None),
        P(("seq", "batch"), None),
        P(("seq", "batch"), None),
    )
    return jax.shard_map(body, mesh=mesh, in_specs=in_specs, out_specs=out_specs, check_vma=False)
```

```python
import functools
import math

import jax
import jax.numpy as jnp
from jax import lax
from jax.experimental import pallas as pl
from jax.experimental.pallas import tpu as pltpu
from jax.sharding import PartitionSpec as P

H = 8
DK = 16
DV = 128
F = 160
T = 128
N = 64
PART = F // 8
D = 2048
UNITS = 20
MESH = pl.DeviceIdType.MESH
BF = jnp.bfloat16
F32 = jnp.float32
ROOT = 1.0 / math.sqrt(2.0)
HBM = pl.BlockSpec(memory_space=pl.ANY)
VMEM = pl.BlockSpec(memory_space=pltpu.VMEM)


def dot(left, right, dims=(1, 0)):
    return lax.dot_general(left, right, ((dims[:1], dims[1:]), ((), ())), preferred_element_type=F32)


def halves(a):
    high = a.astype(BF)
    return high, (a - high.astype(F32)).astype(BF)


def dot2(pair, right, dims=(1, 0)):
    return dot(pair[0], right, dims) + dot(pair[1], right, dims)


def dot2r(left, pair, dims=(1, 0)):
    return dot(left, pair[0], dims) + dot(left, pair[1], dims)


def dot3(lefts, rights, dims=(1, 0)):
    return (
        dot(lefts[0], rights[0], dims)
        + dot(lefts[0], rights[1], dims)
        + dot(lefts[1], rights[0], dims)
    )


def ahead(a, d):
    return pltpu.roll(a, (8 - d) % 8, 0) if d % 8 else a


def back(a, d):
    return pltpu.roll(a, d, 0) if d % 8 else a


def phi(u):
    row = lax.broadcasted_iota(jnp.int32, (8, T), 0)
    low, high = u[:8], u[8:]
    tiles = []
    for m, fill in ((low, jnp.zeros((8, T), F32)), (high, (row == 4).astype(F32))):
        tiles.append(m * m * ROOT)
        for d in range(1, 4):
            tiles.append(m * ahead(m, d))
        tiles.append(jnp.where(row < 4, m * ahead(m, 4), fill))
    for d in range(8):
        tiles.append(low * ahead(high, d))
    return jnp.concatenate(tiles + [low, high], 0)


def pull(u, grad):
    row = lax.broadcasted_iota(jnp.int32, (8, T), 0)
    low, high = u[:8], u[8:]
    tile = lambda n: grad[8 * n : 8 * n + 8]
    sums = []
    for at, m in ((0, low), (5, high)):
        total = tile(18 + at // 5) + tile(at) * (2.0 * ROOT) * m
        for d in range(1, 5):
            piece = tile(at + d)
            if d == 4:
                piece = jnp.where(row < 4, piece, 0.0)
            total = total + piece * ahead(m, d) + back(piece * m, d)
        sums.append(total)
    for d in range(8):
        piece = tile(10 + d)
        sums[0] = sums[0] + piece * ahead(high, d)
        sums[1] = sums[1] + back(piece * low, d)
    return jnp.concatenate(sums, 0)


def kernel(
    x_hbm, c_hbm, wq_hbm, wk_hbm, wv_hbm, gi_ref, o_ref,
    x_ref, c_ref, wq_ref, wk_ref, wv_ref,
    uq_ref, uk_ref, fqt, fkt, fqn, fkn, v_ref, ath, atl, ni_ref, rd_ref, gnh, gnl, ga_ref,
    gv_ref, gk_ref, sh_ref, gt_ref,
    s1, s2, s3, s4, t1, t2, t3, t4, nsrc, nrcv, tsrc, trcv,
    xt_ref, xr_ref, xp_ref, gs_ref, gr_ref, gp_ref,
    p_ref, a_ref, b_ref, q_ref, r2_ref, w_ref, r3_ref,
    load, a2s, a2r, lns, lnr, xs, xr, gss, grr, p1s, p1r, p2s, p2r, p3s, p3r,
):
    me = lax.axis_index("seq")
    core = lax.axis_index("batch")
    other = 1 - core
    at = (me // 16, (me // 4) % 4, me % 4)
    weight = (16, 4, 1)

    def along(d, c):
        return (me + (c - at[d]) * weight[d], core)

    def copy_to(src, dst, send, recv, device):
        return pltpu.make_async_remote_copy(
            src_ref=src, dst_ref=dst, send_sem=send, recv_sem=recv,
            device_id=device, device_id_type=MESH,
        )

    def push(src, dst, send, recv, device):
        copy = copy_to(src, dst, send, recv, device)
        copy.start()
        return copy

    def drain(ref, sem):
        copy_to(ref, ref, sem, sem, (me, other)).wait_send()

    loads = []
    for n, (src, dst) in enumerate(
        ((x_hbm, x_ref), (wk_hbm, wk_ref), (wq_hbm, wq_ref), (wv_hbm, wv_ref), (c_hbm, c_ref))
    ):
        copy = pltpu.make_async_copy(src, dst, load.at[n])
        copy.start()
        loads.append(copy)

    barrier = pltpu.get_barrier_semaphore()

    def greet(k, carry):
        pl.semaphore_signal(barrier, inc=1, device_id=((me + k) % N, core), device_id_type=MESH)
        return carry

    lax.fori_loop(1, N, greet, 0)
    pl.semaphore_signal(barrier, inc=1, device_id=(me, other), device_id_type=MESH)

    def scatter(src, dst, n):
        def step(k, carry):
            peer = (me + k) % N
            copy_to(src.at[peer], dst.at[me], a2s.at[n], a2r.at[n, me], (peer, core)).start()
            return carry

        lax.fori_loop(1, N, step, 0)
        dst[me] = src[me]

    def arrive(dst, n, j):
        @pl.when(j != me)
        def _():
            copy_to(dst.at[j], dst.at[j], a2s.at[n], a2r.at[n, j], (j, core)).wait_recv()

    def scan(src, dst, n, reverse):
        def step(i, run):
            j = N - 1 - i if reverse else i
            arrive(src, n, j)
            dst[j] = run
            return run + src[j]

        lax.fori_loop(0, N, step, jnp.zeros((PART, DV), F32))

    def arrive_all(dst, n):
        def step(j, carry):
            arrive(dst, n, j)
            return carry

        lax.fori_loop(0, N, step, 0)

    def put_state(dst, h, value):
        for j in range(8):
            dst[8 * h + j, :16, :] = value[16 * j : 16 * j + 16]
            dst[8 * h + j, 16:, :] = value[128 + 4 * j : 132 + 4 * j]

    def get_state(src, h):
        tiles = [src[8 * h + j, :16, :] for j in range(8)]
        tiles += [src[8 * h + j, 16:, :] for j in range(8)]
        return jnp.concatenate(tiles, 0)

    def line_send(src, rcv, n, d):
        for k in range(1, 4):
            c = (at[d] + k) % 4
            push(src.at[d], rcv.at[d, at[d]], lns.at[n, d], lnr.at[n, d], along(d, c))

    def line_sum(src, rcv, n, d, reverse):
        block = rcv.at[d, pl.ds(0, 3)]
        copy_to(block, block, lns.at[n, d], lnr.at[n, d], (me, other)).wait_recv()
        rcv[d, at[d]] = src[d]
        total = jnp.zeros((8, 256), F32)
        part = jnp.zeros((8, 256), F32)
        for c in range(4):
            block = rcv[d, c]
            total = total + block
            keep = c > at[d] if reverse else c < at[d]
            part = part + jnp.where(keep, block, 0.0)
        return total, part

    causal = lax.broadcasted_iota(jnp.int32, (T, T), 0) >= lax.broadcasted_iota(jnp.int32, (T, T), 1)
    anti = lax.broadcasted_iota(jnp.int32, (T, T), 0) <= lax.broadcasted_iota(jnp.int32, (T, T), 1)
    lane = lax.broadcasted_iota(jnp.int32, (T, DV), 1)
    ones = jnp.ones((T, DV), BF)
    rows8 = lax.broadcasted_iota(jnp.int32, (8, F), 0)

    loads[0].wait()
    loads[1].wait()
    x = x_ref[...]
    flat = dot(x, wk_ref[...]).T * 0.5
    norm = jnp.zeros((8, F), F32)
    for h in range(H):
        u = flat[DK * h : DK * h + DK]
        uk_ref[h] = u
        f = phi(u)
        ft = f.astype(BF)
        fkt[h] = ft
        fkn[h] = f.T.astype(BF)
        norm = jnp.where(rows8 == h, dot(jnp.ones((8, T), BF), ft, (1, 1)), norm)
    nsrc[2] = jnp.concatenate([norm, jnp.zeros((8, 256 - F), F32)], 1)
    pl.semaphore_wait(barrier, N)
    line_send(nsrc, nrcv, 0, 2)

    loads[3].wait()
    for h in range(H):
        val = dot(x, wv_ref[:, h * DV : (h + 1) * DV]).astype(BF)
        v_ref[h] = val
        put_state(s1, h, dot(fkt[h], val))

    total, prefix = line_sum(nsrc, nrcv, 0, 2, False)
    nsrc[1] = total
    line_send(nsrc, nrcv, 0, 1)

    loads[2].wait()
    flat = dot(x, wq_ref[...]).T * 0.5
    for h in range(H):
        u = flat[DK * h : DK * h + DK]
        uq_ref[h] = u
        f = phi(u)
        fqt[h] = f.astype(BF)
        fqn[h] = f.T.astype(BF)

    total, part = line_sum(nsrc, nrcv, 0, 1, False)
    prefix = prefix + part
    nsrc[0] = total
    line_send(nsrc, nrcv, 0, 0)
    scatter(s1, s2, 0)

    def inside(h):
        attn = halves(jnp.where(causal, dot(fqn[h], fkt[h]), 0.0))
        both = dot2(attn, jnp.concatenate([v_ref[h], ones], 1))
        ni_ref[h] = both[:, :DV]
        rd_ref[h] = both[:, DV:]
        turned = halves(jnp.where(anti, dot(fkn[h], fqt[h]), 0.0))
        ath[h] = turned[0]
        atl[h] = turned[1]

    for h in range(H):
        inside(h)
    total, part = line_sum(nsrc, nrcv, 0, 0, False)
    prefix = prefix + part
    loads[4].wait()

    for h in range(H):
        row = halves(jnp.broadcast_to(prefix[h : h + 1, :F], (DV, F)))
        den = rd_ref[h] + dot2r(fqn[h], row, (1, 1))
        scale = 1.0 / den
        rd_ref[h] = scale
        numer = c_ref[:, h * DV : (h + 1) * DV].astype(F32) * scale
        gn = halves(numer)
        gnh[h] = gn[0]
        gnl[h] = gn[1]
        put_state(t1, h, dot2r(fqt[h], gn))
    scatter(t1, t2, 2)

    for h in range(H):
        gn = (gnh[h], gnl[h])
        gv_ref[h] = dot3((ath[h], atl[h]), gn)
        ga_ref[h] = dot2(gn, v_ref[h], (1, 1))

    scan(s2, s3, 0, False)
    scatter(s3, s4, 1)

    for b in range(D // 128):
        block = x_ref[:, b * 128 : (b + 1) * 128].astype(F32).T
        for i in range(4):
            for half in range(2):
                row = 32 * i + 16 * half
                xt_ref[half, 4 * b + i] = block[row : row + 16]
    swap = push(xt_ref.at[other], xr_ref, xs.at[0], xr.at[0], (me, other))
    xp_ref[:, :T] = xt_ref[core].reshape(D // 2, T).astype(BF)

    scan(t2, t3, 2, True)
    scatter(t3, t4, 3)

    turned = jnp.concatenate([prefix, jnp.zeros((T - 8, 256), F32)], 0).T[:F]
    columns = halves(turned)
    arrive_all(s4, 1)
    down = jnp.zeros((F, DV), F32)
    grads = []
    for h in range(H):
        state = halves(get_state(s4, h))
        gn = (gnh[h], gnl[h])
        num = ni_ref[h] + dot2r(fqn[h], state)
        numer = gn[0].astype(F32) + gn[1].astype(F32)
        denom = -jnp.sum(numer * num, 1, keepdims=True) * rd_ref[h]
        ga = halves(jnp.where(causal, ga_ref[h] + denom, 0.0))
        mine = halves(jnp.where(lane == h, denom, 0.0))
        left = [jnp.concatenate([s, c], 1) for s, c in zip(state, columns)]
        right = [jnp.concatenate([g, m], 1) for g, m in zip(gn, mine)]
        gfq = dot2r(fkt[h], ga, (1, 1)) + dot3(left, right, (1, 1))
        grads.append(pull(uq_ref[h], gfq) * 0.5)
        gk_ref[h] = dot2r(fqt[h], ga)
        down = down + dot2r(fqt[h], mine)
    rows = jnp.concatenate([down, jnp.zeros((256 - F, DV), F32)], 0).T
    tsrc[2] = rows[:8]
    line_send(tsrc, trcv, 1, 2)
    grad_q = jnp.concatenate(grads, 0).T.astype(BF)

    def share(m, value):
        gp_ref[:T, 256 * m : 256 * m + 256] = value
        gs_ref[m] = value.astype(F32)
        return push(gs_ref.at[m], gr_ref.at[m], gss.at[0], grr.at[m], (me, other))

    arrive_all(t4, 3)
    shares = []
    for m in range(4):
        pieces = []
        for h in (2 * m, 2 * m + 1):
            state = halves(get_state(t4, h))
            sh_ref[h] = state[0]
            gt_ref[h] = state[1]
            pieces.append((gv_ref[h] + dot2r(fkn[h], state)).astype(BF))
        shares.append(share(m, jnp.concatenate(pieces, 1)))

    total, suffix = line_sum(tsrc, trcv, 1, 2, True)
    tsrc[1] = total
    line_send(tsrc, trcv, 1, 1)

    swap.wait_recv()
    xp_ref[:, T:] = xr_ref[...].reshape(D // 2, T).astype(BF)

    def multiply(m):
        shares[m].wait_recv()
        gp_ref[T:, 256 * m : 256 * m + 256] = gr_ref[m].astype(BF)
        right = gp_ref[:, 256 * m : 256 * m + 256]
        for z in range(4):
            part = dot(xp_ref[256 * z : 256 * z + 256, :], right)
            for i in range(2):
                block = part[:, i * DV : (i + 1) * DV].reshape(4, 4, 2, 8, DV)
                for r in range(2):
                    p_ref[4 * m + 2 * i + r, z] = block[:, :, r]

    def line_part(u, g, c, half):
        take = pl.ds(2 * half, 2)
        if g == 0:
            return (u, c, take)
        if g == 1:
            return (u, take, c)
        return (u, take, slice(None), c)

    def arrived(ref, sem):
        copy_to(ref, ref, sem, sem, (me, other)).wait_recv()

    def stage0(u):
        g = u % 3
        i = at[g]
        right, left, far = (i + 1) % 4, (i + 3) % 4, (i + 2) % 4
        keys = (
            (far, 0, right, a_ref.at[u, 0]),
            (far, 1, left, a_ref.at[u, 1]),
            (right, 1, right, b_ref.at[u, 0, pl.ds(2, 2)]),
            (left, 0, left, b_ref.at[u, 1, pl.ds(0, 2)]),
        )
        for n, (c, half, peer, dst) in enumerate(keys):
            push(p_ref.at[line_part(u, g, c, half)], dst, p1s.at[0], p1r.at[u, n // 2], along(g, peer))

    def stage1(u):
        g = u % 3
        i = at[g]
        right, left = (i + 1) % 4, (i + 3) % 4
        arrived(a_ref.at[u], p1r.at[u, 0])
        for n, (peer, half) in enumerate(((right, 0), (left, 1))):
            where = line_part(u, g, peer, half)
            p_ref[where] = p_ref[where] + a_ref[u, n]
            dst = b_ref.at[u, n, pl.ds(2 * half, 2)]
            push(p_ref.at[where], dst, p1s.at[1], p1r.at[u, 1], along(g, peer))

    order = ((1, 2), (2, 0), (0, 1))

    def stage2(u):
        g = u % 3
        arrived(b_ref.at[u], p1r.at[u, 1])
        for half in range(2):
            mine = p_ref[line_part(u, g, at[g], half)]
            mine = mine + b_ref[u, 0, 2 * half : 2 * half + 2] + b_ref[u, 1, 2 * half : 2 * half + 2]
            for i in range(2):
                if g == 1:
                    q_ref[u, :, 2 * half + i] = mine[i]
                else:
                    q_ref[u, 2 * half + i] = mine[i]
        d = order[g][0]
        for k in range(1, 4):
            c = (at[d] + k) % 4
            push(q_ref.at[u, c], r2_ref.at[u, at[d]], p2s.at[0], p2r.at[u], along(d, c))

    def from_line(d, src, dst, recv, u):
        arrived(dst.at[u, pl.ds(0, 3)], recv.at[u])
        total = src[u, at[d]]
        for k in range(1, 4):
            total = total + dst[u, (at[d] + k) % 4]
        return total

    def stage3(u):
        d, e = order[u % 3]
        w_ref[u] = from_line(d, q_ref, r2_ref, p2r, u)
        for k in range(1, 4):
            c = (at[e] + k) % 4
            push(w_ref.at[u, c], r3_ref.at[u, at[e]], p3s.at[0], p3r.at[u], along(e, c))

    def stage4(u):
        total = from_line(order[u % 3][1], w_ref, r3_ref, p3r, u)
        piece, r = u // 2, u % 2
        rows = slice(8 * r, 8 * r + 8)
        o_ref[rows, piece * DV : (piece + 1) * DV] = total

    multiply(0)
    for u in range(4):
        stage0(u)
    multiply(1)
    for u in range(4, 8):
        stage0(u)

    total, part = line_sum(tsrc, trcv, 1, 1, True)
    suffix = suffix + part
    tsrc[0] = total
    line_send(tsrc, trcv, 1, 0)

    multiply(2)
    for u in range(8, 12):
        stage0(u)
    multiply(3)
    for u in range(12, 16):
        stage0(u)
    for u in range(6):
        stage1(u)

    total, part = line_sum(tsrc, trcv, 1, 0, True)
    suffix = suffix + part
    turned = jnp.concatenate([suffix, jnp.zeros((T - 8, 256), F32)], 0).T[:F]
    grads = []
    for h in range(H):
        gfk = gk_ref[h] + dot2((sh_ref[h], gt_ref[h]), v_ref[h], (1, 1)) + turned[:, h : h + 1]
        grads.append(pull(uk_ref[h], gfk) * 0.5)
    grad_k = jnp.concatenate(grads, 0).T.astype(BF)
    shares.append(share(4, jnp.concatenate([grad_q, grad_k], 1)))
    for u in range(6, 12):
        stage1(u)
    multiply(4)
    for u in range(16, 20):
        stage0(u)
    for u in range(12, 16):
        stage1(u)

    wide = D // 8

    def inputs(n):
        cut = slice(n * wide, (n + 1) * wide)
        total = dot(gp_ref[:T, : H * DV], wv_ref[cut, :], (1, 1))
        total = total + dot(gp_ref[:T, H * DV : H * DV + 128], wq_ref[cut, :], (1, 1))
        total = total + dot(gp_ref[:T, H * DV + 128 :], wk_ref[cut, :], (1, 1))
        gi_ref[:, cut] = total.astype(BF)

    for n in range(2):
        inputs(n)
    for u in range(8):
        stage2(u)
    for n in range(2, 4):
        inputs(n)
    for u in range(16, 20):
        stage1(u)
    for n in range(4, 6):
        inputs(n)
    for u in range(8, 16):
        stage2(u)
    for u in range(8):
        stage3(u)
    for n in range(6, 8):
        inputs(n)
    for u in range(16, 20):
        stage2(u)
    for u in range(8, 16):
        stage3(u)
    for u in range(8):
        stage4(u)
    for u in range(16, 20):
        stage3(u)
    for u in range(8, 20):
        stage4(u)
    for n, src in enumerate((s1, s3, t1, t3)):
        drain(src.at[pl.ds(0, N - 1)], a2s.at[n])
    for n, rcv in enumerate((nrcv, trcv)):
        for d in range(3):
            drain(rcv.at[d, pl.ds(0, 3)], lns.at[n, d])
    drain(xr_ref, xs.at[0])
    drain(gr_ref, gss.at[0])
    drain(b_ref, p1s.at[0])
    drain(a_ref, p1s.at[1])
    drain(q_ref.at[:, pl.ds(0, 3)], p2s.at[0])
    drain(w_ref.at[:, pl.ds(0, 3)], p3s.at[0])


def results(gi_in, w_in, gi_ref, oq_ref, ok_ref, ov_ref, g_ref, w_ref, load, save):
    reads = [
        pltpu.make_async_copy(gi_in, g_ref, load.at[0]),
        pltpu.make_async_copy(w_in, w_ref, load.at[1]),
    ]
    for copy in reads:
        copy.start()
    reads[1].wait()
    writes = [
        pltpu.make_async_copy(w_ref.at[:, pl.ds(0, H * DV)], ov_ref, save.at[0]),
        pltpu.make_async_copy(w_ref.at[:, pl.ds(H * DV, 128)], oq_ref, save.at[1]),
        pltpu.make_async_copy(w_ref.at[:, pl.ds(H * DV + 128, 128)], ok_ref, save.at[2]),
    ]
    for copy in writes:
        copy.start()
    reads[0].wait()
    writes.append(pltpu.make_async_copy(g_ref, gi_ref, save.at[3]))
    writes[3].start()
    for copy in writes:
        copy.wait()


def body(inputs, cotangent, w_query, w_key, w_value):
    vm = lambda *shape: pltpu.VMEM(shape, F32)
    vb = lambda *shape: pltpu.VMEM(shape, BF)
    sems = lambda *sizes: pltpu.SemaphoreType.DMA(sizes)
    state = lambda: vm(N, PART, DV)
    scratch = [
        vb(T, D), vb(T, H * DV), vb(D, 128), vb(D, 128), vb(D, H * DV),
        vm(H, DK, T), vm(H, DK, T), vb(H, F, T), vb(H, F, T), vb(H, T, F), vb(H, T, F), vb(H, T, DV),
        vb(H, T, T), vb(H, T, T), vm(H, T, DV), vm(H, T, DV), vb(H, T, DV), vb(H, T, DV), vm(H, T, T),
        vm(H, T, DV), vm(H, F, T), vb(H, F, DV), vb(H, F, DV),
        state(), state(), state(), state(), state(), state(), state(), state(),
        vm(3, 8, 256), vm(3, 4, 8, 256), vm(3, 8, 256), vm(3, 4, 8, 256),
        vm(2, N, 16, T), vm(N, 16, T), vb(D // 2, 2 * T), vm(5, T, 256), vm(5, T, 256), vb(2 * T, 1280),
        vm(UNITS, 4, 4, 4, 8, DV), vm(UNITS, 2, 2, 4, 8, DV), vm(UNITS, 2, 4, 4, 8, DV),
        vm(UNITS, 4, 4, 8, DV), vm(UNITS, 4, 4, 8, DV), vm(UNITS, 4, 8, DV), vm(UNITS, 4, 8, DV),
        sems(5), sems(4), sems(4, N), sems(2, 3), sems(2, 3), sems(1), sems(1), sems(1), sems(5),
        sems(2), sems(UNITS, 2), sems(1), sems(UNITS), sems(1), sems(UNITS),
    ]
    grad_in, grad_w = pl.pallas_call(
        kernel,
        out_shape=[jax.ShapeDtypeStruct((T, D), BF), jax.ShapeDtypeStruct((16, 1280), F32)],
        in_specs=[HBM] * 5,
        out_specs=[VMEM] * 2,
        scratch_shapes=scratch,
        compiler_params=pltpu.CompilerParams(
            collective_id=0, has_side_effects=True, vmem_limit_bytes=60 << 20
        ),
    )(inputs[0], cotangent[0], w_query, w_key, w_value)
    grad_in, grad_wq, grad_wk, grad_wv = pl.pallas_call(
        results,
        out_shape=[
            jax.ShapeDtypeStruct((T, D), BF),
            jax.ShapeDtypeStruct((16, 128), F32),
            jax.ShapeDtypeStruct((16, 128), F32),
            jax.ShapeDtypeStruct((16, H * DV), F32),
        ],
        in_specs=[HBM] * 2,
        out_specs=[HBM] * 4,
        scratch_shapes=[vb(T, D), vm(16, 1280), sems(2), sems(4)],
    )(grad_in, grad_w)
    return (grad_in[None], grad_wq, grad_wk, grad_wv)


def solution(mesh):
    in_specs = (P("batch", "seq", None), P("batch", "seq", None), P(), P(), P())
    out_specs = (
        P("batch", "seq", None),
        P(("seq", "batch"), None),
        P(("seq", "batch"), None),
        P(("seq", "batch"), None),
    )
    return jax.shard_map(body, mesh=mesh, in_specs=in_specs, out_specs=out_specs, check_vma=False)
```

```python
import functools
import math

import jax
import jax.numpy as jnp
from jax import lax
from jax.experimental import pallas as pl
from jax.experimental.pallas import tpu as pltpu
from jax.sharding import PartitionSpec as P

H = 8
DK = 16
DV = 128
F = 160
T = 128
N = 64
PART = F // 8
D = 2048
UNITS = 20
MESH = pl.DeviceIdType.MESH
BF = jnp.bfloat16
F32 = jnp.float32
ROOT = 1.0 / math.sqrt(2.0)
HBM = pl.BlockSpec(memory_space=pl.ANY)
VMEM = pl.BlockSpec(memory_space=pltpu.VMEM)


OFFSETS = sorted(
    ((a, b, c) for a in range(4) for b in range(4) for c in range(4) if a + b + c),
    key=lambda o: -sum(min(v, 4 - v) for v in o),
)


def dot(left, right, dims=(1, 0)):
    return lax.dot_general(left, right, ((dims[:1], dims[1:]), ((), ())), preferred_element_type=F32)


def halves(a):
    high = a.astype(BF)
    return high, (a - high.astype(F32)).astype(BF)


def dot2(pair, right, dims=(1, 0)):
    return dot(pair[0], right, dims) + dot(pair[1], right, dims)


def dot2r(left, pair, dims=(1, 0)):
    return dot(left, pair[0], dims) + dot(left, pair[1], dims)


def dot3(lefts, rights, dims=(1, 0)):
    return (
        dot(lefts[0], rights[0], dims)
        + dot(lefts[0], rights[1], dims)
        + dot(lefts[1], rights[0], dims)
    )


def ahead(a, d):
    return pltpu.roll(a, (8 - d) % 8, 0) if d % 8 else a


def back(a, d):
    return pltpu.roll(a, d, 0) if d % 8 else a


def phi(u):
    row = lax.broadcasted_iota(jnp.int32, (8, T), 0)
    low, high = u[:8], u[8:]
    tiles = []
    for m, fill in ((low, jnp.zeros((8, T), F32)), (high, (row == 4).astype(F32))):
        tiles.append(m * m * ROOT)
        for d in range(1, 4):
            tiles.append(m * ahead(m, d))
        tiles.append(jnp.where(row < 4, m * ahead(m, 4), fill))
    for d in range(8):
        tiles.append(low * ahead(high, d))
    return jnp.concatenate(tiles + [low, high], 0)


def pull(u, grad):
    row = lax.broadcasted_iota(jnp.int32, (8, T), 0)
    low, high = u[:8], u[8:]
    tile = lambda n: grad[8 * n : 8 * n + 8]
    sums = []
    for at, m in ((0, low), (5, high)):
        total = tile(18 + at // 5) + tile(at) * (2.0 * ROOT) * m
        for d in range(1, 5):
            piece = tile(at + d)
            if d == 4:
                piece = jnp.where(row < 4, piece, 0.0)
            total = total + piece * ahead(m, d) + back(piece * m, d)
        sums.append(total)
    for d in range(8):
        piece = tile(10 + d)
        sums[0] = sums[0] + piece * ahead(high, d)
        sums[1] = sums[1] + back(piece * low, d)
    return jnp.concatenate(sums, 0)


def kernel(
    x_hbm, c_hbm, wq_hbm, wk_hbm, wv_hbm, gi_ref, o_ref,
    x_ref, c_ref, wq_ref, wk_ref, wv_ref,
    uq_ref, uk_ref, fqt, fkt, fqn, fkn, v_ref, ath, atl, ni_ref, rd_ref, gnh, gnl, ga_ref,
    gv_ref, gk_ref, sh_ref, gt_ref,
    s1, s2, s3, s4, t1, t2, t3, t4, nsrc, nrcv, tsrc, trcv,
    xt_ref, xr_ref, xp_ref, gs_ref, gr_ref, gp_ref,
    p_ref, a_ref, b_ref, q_ref, r2_ref, w_ref, r3_ref,
    load, a2s, a2r, lns, lnr, xs, xr, gss, grr, p1s, p1r, p2s, p2r, p3s, p3r,
):
    me = lax.axis_index("seq")
    core = lax.axis_index("batch")
    other = 1 - core
    at = (me // 16, (me // 4) % 4, me % 4)
    weight = (16, 4, 1)

    def along(d, c):
        return (me + (c - at[d]) * weight[d], core)

    def copy_to(src, dst, send, recv, device):
        return pltpu.make_async_remote_copy(
            src_ref=src, dst_ref=dst, send_sem=send, recv_sem=recv,
            device_id=device, device_id_type=MESH,
        )

    def push(src, dst, send, recv, device):
        copy = copy_to(src, dst, send, recv, device)
        copy.start()
        return copy

    def drain(ref, sem):
        copy_to(ref, ref, sem, sem, (me, other)).wait_send()

    loads = []
    for n, (src, dst) in enumerate(
        ((x_hbm, x_ref), (wk_hbm, wk_ref), (wq_hbm, wq_ref), (wv_hbm, wv_ref), (c_hbm, c_ref))
    ):
        copy = pltpu.make_async_copy(src, dst, load.at[n])
        copy.start()
        loads.append(copy)

    barrier = pltpu.get_barrier_semaphore()

    def greet(k, carry):
        pl.semaphore_signal(barrier, inc=1, device_id=((me + k) % N, core), device_id_type=MESH)
        return carry

    lax.fori_loop(1, N, greet, 0)
    pl.semaphore_signal(barrier, inc=1, device_id=(me, other), device_id_type=MESH)

    def peers():
        part = [[(at[d] + k) % 4 * weight[d] for k in range(4)] for d in range(3)]
        return [part[0][a] + part[1][b] + part[2][c] for a, b, c in OFFSETS]

    def scatter(src, dst, n):
        for peer in peers():
            copy_to(src.at[peer], dst.at[me], a2s.at[n], a2r.at[n, me], (peer, core)).start()
        dst[me] = src[me]

    def arrive(dst, n, j):
        @pl.when(j != me)
        def _():
            copy_to(dst.at[j], dst.at[j], a2s.at[n], a2r.at[n, j], (j, core)).wait_recv()

    def scan(src, dst, n, reverse):
        def step(i, run):
            j = N - 1 - i if reverse else i
            arrive(src, n, j)
            dst[j] = run
            return run + src[j]

        lax.fori_loop(0, N, step, jnp.zeros((PART, DV), F32))

    def arrive_all(dst, n):
        def step(j, carry):
            arrive(dst, n, j)
            return carry

        lax.fori_loop(0, N, step, 0)

    def put_state(dst, h, value):
        for j in range(8):
            dst[8 * h + j, :16, :] = value[16 * j : 16 * j + 16]
            dst[8 * h + j, 16:, :] = value[128 + 4 * j : 132 + 4 * j]

    def get_state(src, h):
        tiles = [src[8 * h + j, :16, :] for j in range(8)]
        tiles += [src[8 * h + j, 16:, :] for j in range(8)]
        return jnp.concatenate(tiles, 0)

    def gather(src, rcv, n):
        for peer in peers():
            copy_to(src, rcv.at[me], lns.at[n], lnr.at[n], (peer, core)).start()
        rcv[me] = src[...]

    def gathered(rcv, n, low, high):
        blocks = rcv.at[pl.ds(0, N - 1)]
        copy_to(blocks, blocks, lns.at[n], lnr.at[n], (me, other)).wait_recv()

        def step(j, total):
            return total + rcv[j]

        total = lax.fori_loop(low, high, step, jnp.zeros((10, DV), F32))
        rows = []
        for h in range(H):
            at_lane = 32 * (h % 4)
            rest = total[8 + h // 4 : 9 + h // 4, at_lane : at_lane + 32]
            rows.append(jnp.concatenate([total[h : h + 1], rest], 1))
        return jnp.concatenate(rows, 0)

    def turn(rows):
        wide = jnp.concatenate([rows, jnp.zeros((8, 256 - F), F32)], 1)
        return jnp.concatenate([wide, jnp.zeros((T - 8, 256), F32)], 0).T[:F]

    causal = lax.broadcasted_iota(jnp.int32, (T, T), 0) >= lax.broadcasted_iota(jnp.int32, (T, T), 1)
    anti = lax.broadcasted_iota(jnp.int32, (T, T), 0) <= lax.broadcasted_iota(jnp.int32, (T, T), 1)
    lane = lax.broadcasted_iota(jnp.int32, (T, DV), 1)
    ones = jnp.ones((T, DV), BF)
    rows8 = lax.broadcasted_iota(jnp.int32, (8, DV), 0)

    loads[0].wait()
    loads[1].wait()
    x = x_ref[...]
    flat = dot(x, wk_ref[...]).T * 0.5
    norm = jnp.zeros((8, DV), F32)
    one = jnp.ones((8, T), BF)
    for h in range(H):
        u = flat[DK * h : DK * h + DK]
        uk_ref[h] = u
        f = phi(u)
        ft = f.astype(BF)
        fkt[h] = ft
        fkn[h] = f.T.astype(BF)
        norm = jnp.where(rows8 == h, dot(one, ft[:DV], (1, 1)), norm)
    nsrc[:8] = norm
    for i in range(2):
        last = jnp.concatenate([fkt[h, DV:] for h in range(4 * i, 4 * i + 4)], 0)
        nsrc[8 + i : 9 + i] = dot(one, last, (1, 1))[:1]
    pl.semaphore_wait(barrier, N)
    gather(nsrc, nrcv, 0)

    loads[3].wait()
    for m in range(4):
        both = dot(x, wv_ref[:, 256 * m : 256 * m + 256]).astype(BF)
        for i in range(2):
            val = both[:, i * DV : (i + 1) * DV]
            v_ref[2 * m + i] = val
            put_state(s1, 2 * m + i, dot(fkt[2 * m + i], val))
    loads[2].wait()
    flat = dot(x, wq_ref[...]).T * 0.5
    for h in range(H):
        u = flat[DK * h : DK * h + DK]
        uq_ref[h] = u
        f = phi(u)
        fqt[h] = f.astype(BF)
        fqn[h] = f.T.astype(BF)

    def inside(h):
        attn = halves(jnp.where(causal, dot(fqn[h], fkt[h]), 0.0))
        both = dot2(attn, jnp.concatenate([v_ref[h], ones], 1))
        ni_ref[h] = both[:, :DV]
        rd_ref[h] = both[:, DV:]
        turned = halves(jnp.where(anti, dot(fkn[h], fqt[h]), 0.0))
        ath[h] = turned[0]
        atl[h] = turned[1]

    for h in range(H):
        inside(h)
    scatter(s1, s2, 0)
    prefix = gathered(nrcv, 0, 0, me)
    loads[4].wait()

    for h in range(H):
        row = halves(jnp.broadcast_to(prefix[h : h + 1], (DV, F)))
        den = rd_ref[h] + dot2r(fqn[h], row, (1, 1))
        scale = 1.0 / den
        rd_ref[h] = scale
        numer = c_ref[:, h * DV : (h + 1) * DV].astype(F32) * scale
        gn = halves(numer)
        gnh[h] = gn[0]
        gnl[h] = gn[1]
        put_state(t1, h, dot2r(fqt[h], gn))
    scatter(t1, t2, 2)

    for h in range(H):
        gn = (gnh[h], gnl[h])
        gv_ref[h] = dot3((ath[h], atl[h]), gn)
        ga_ref[h] = dot2(gn, v_ref[h], (1, 1))

    scan(s2, s3, 0, False)
    scatter(s3, s4, 1)

    for b in range(D // 128):
        block = x_ref[:, b * 128 : (b + 1) * 128].astype(F32).T
        for i in range(4):
            for half in range(2):
                row = 32 * i + 16 * half
                xt_ref[half, 4 * b + i] = block[row : row + 16]
    swap = push(xt_ref.at[other], xr_ref, xs.at[0], xr.at[0], (me, other))
    xp_ref[:, :T] = xt_ref[core].reshape(D // 2, T).astype(BF)

    scan(t2, t3, 2, True)
    scatter(t3, t4, 3)

    def share(m, value):
        gp_ref[:T, 256 * m : 256 * m + 256] = value
        gs_ref[m] = value.astype(F32)
        return push(gs_ref.at[m], gr_ref.at[m], gss.at[0], grr.at[m], (me, other))

    turned = turn(prefix)
    columns = halves(turned)
    arrive_all(s4, 1)
    down = jnp.zeros((F, DV), F32)
    grads = []
    for h in range(H):
        state = halves(get_state(s4, h))
        gn = (gnh[h], gnl[h])
        num = ni_ref[h] + dot2r(fqn[h], state)
        numer = gn[0].astype(F32) + gn[1].astype(F32)
        denom = -jnp.sum(numer * num, 1, keepdims=True) * rd_ref[h]
        ga = halves(jnp.where(causal, ga_ref[h] + denom, 0.0))
        mine = halves(jnp.where(lane == h, denom, 0.0))
        left = [jnp.concatenate([s, c], 1) for s, c in zip(state, columns)]
        right = [jnp.concatenate([g, m], 1) for g, m in zip(gn, mine)]
        gfq = dot2r(fkt[h], ga, (1, 1)) + dot3(left, right, (1, 1))
        grads.append(pull(uq_ref[h], gfq) * 0.5)
        gk_ref[h] = dot2r(fqt[h], ga)
        down = down + dot2r(fqt[h], mine)
    rows = jnp.concatenate([down, jnp.zeros((256 - F, DV), F32)], 0).T
    tsrc[:8] = rows[:8, :DV]
    for i in range(2):
        tsrc[8 + i : 9 + i] = jnp.concatenate(
            [rows[h : h + 1, DV:F] for h in range(4 * i, 4 * i + 4)], 1
        )
    gather(tsrc, trcv, 1)
    grad_q = jnp.concatenate(grads, 0).T.astype(BF)

    arrive_all(t4, 3)
    shares = []
    for m in range(4):
        pieces = []
        for h in (2 * m, 2 * m + 1):
            state = halves(get_state(t4, h))
            sh_ref[h] = state[0]
            gt_ref[h] = state[1]
            pieces.append((gv_ref[h] + dot2r(fkn[h], state)).astype(BF))
        shares.append(share(m, jnp.concatenate(pieces, 1)))

    swap.wait_recv()
    xp_ref[:, T:] = xr_ref[...].reshape(D // 2, T).astype(BF)

    def multiply(m):
        shares[m].wait_recv()
        gp_ref[T:, 256 * m : 256 * m + 256] = gr_ref[m].astype(BF)
        right = gp_ref[:, 256 * m : 256 * m + 256]
        for z in range(4):
            part = dot(xp_ref[256 * z : 256 * z + 256, :], right)
            for i in range(2):
                block = part[:, i * DV : (i + 1) * DV].reshape(4, 4, 2, 8, DV)
                for r in range(2):
                    p_ref[4 * m + 2 * i + r, z] = block[:, :, r]

    def line_part(u, g, c, half):
        take = pl.ds(2 * half, 2)
        if g == 0:
            return (u, c, take)
        if g == 1:
            return (u, take, c)
        return (u, take, slice(None), c)

    def arrived(ref, sem):
        copy_to(ref, ref, sem, sem, (me, other)).wait_recv()

    def stage0(u):
        g = u % 3
        i = at[g]
        right, left, far = (i + 1) % 4, (i + 3) % 4, (i + 2) % 4
        keys = (
            (far, 0, right, a_ref.at[u, 0]),
            (far, 1, left, a_ref.at[u, 1]),
            (right, 1, right, b_ref.at[u, 0, pl.ds(2, 2)]),
            (left, 0, left, b_ref.at[u, 1, pl.ds(0, 2)]),
        )
        for n, (c, half, peer, dst) in enumerate(keys):
            push(p_ref.at[line_part(u, g, c, half)], dst, p1s.at[0], p1r.at[u, n // 2], along(g, peer))

    def stage1(u):
        g = u % 3
        i = at[g]
        right, left = (i + 1) % 4, (i + 3) % 4
        arrived(a_ref.at[u], p1r.at[u, 0])
        for n, (peer, half) in enumerate(((right, 0), (left, 1))):
            where = line_part(u, g, peer, half)
            p_ref[where] = p_ref[where] + a_ref[u, n]
            dst = b_ref.at[u, n, pl.ds(2 * half, 2)]
            push(p_ref.at[where], dst, p1s.at[1], p1r.at[u, 1], along(g, peer))

    order = ((1, 2), (2, 0), (0, 1))

    def stage2(u):
        g = u % 3
        arrived(b_ref.at[u], p1r.at[u, 1])
        for half in range(2):
            mine = p_ref[line_part(u, g, at[g], half)]
            mine = mine + b_ref[u, 0, 2 * half : 2 * half + 2] + b_ref[u, 1, 2 * half : 2 * half + 2]
            for i in range(2):
                if g == 1:
                    q_ref[u, :, 2 * half + i] = mine[i]
                else:
                    q_ref[u, 2 * half + i] = mine[i]
        d = order[g][0]
        for k in range(1, 4):
            c = (at[d] + k) % 4
            push(q_ref.at[u, c], r2_ref.at[u, at[d]], p2s.at[0], p2r.at[u], along(d, c))

    def from_line(d, src, dst, recv, u):
        arrived(dst.at[u, pl.ds(0, 3)], recv.at[u])
        total = src[u, at[d]]
        for k in range(1, 4):
            total = total + dst[u, (at[d] + k) % 4]
        return total

    def stage3(u):
        d, e = order[u % 3]
        w_ref[u] = from_line(d, q_ref, r2_ref, p2r, u)
        for k in range(1, 4):
            c = (at[e] + k) % 4
            push(w_ref.at[u, c], r3_ref.at[u, at[e]], p3s.at[0], p3r.at[u], along(e, c))

    def stage4(u):
        total = from_line(order[u % 3][1], w_ref, r3_ref, p3r, u)
        piece, r = u // 2, u % 2
        rows = slice(8 * r, 8 * r + 8)
        o_ref[rows, piece * DV : (piece + 1) * DV] = total

    for m in range(2):
        multiply(m)
        for u in range(4 * m, 4 * m + 4):
            stage0(u)
    suffix = gathered(trcv, 1, me + 1, N)
    turned = turn(suffix)
    grads = []
    for h in range(H):
        gfk = gk_ref[h] + dot2((sh_ref[h], gt_ref[h]), v_ref[h], (1, 1)) + turned[:, h : h + 1]
        grads.append(pull(uk_ref[h], gfk) * 0.5)
    grad_k = jnp.concatenate(grads, 0).T.astype(BF)
    shares.append(share(4, jnp.concatenate([grad_q, grad_k], 1)))
    for m in range(2, 5):
        multiply(m)
        for u in range(4 * m, 4 * m + 4):
            stage0(u)
    wide = D // 8

    def inputs(n):
        cut = slice(n * wide, (n + 1) * wide)
        total = dot(gp_ref[:T, : H * DV], wv_ref[cut, :], (1, 1))
        total = total + dot(gp_ref[:T, H * DV : H * DV + 128], wq_ref[cut, :], (1, 1))
        total = total + dot(gp_ref[:T, H * DV + 128 :], wk_ref[cut, :], (1, 1))
        gi_ref[:, cut] = total.astype(BF)

    for n in range(4):
        inputs(n)
    for u in range(8):
        stage1(u)
    for n in range(4, 8):
        inputs(n)
    for u in range(8, 20):
        stage1(u)
        if u >= 14:
            stage2(u - 14)
    for u in range(6, 20):
        stage2(u)
        if u >= 12:
            stage3(u - 12)
    for u in range(8, 20):
        stage3(u)
        if u >= 14:
            stage4(u - 14)
    for u in range(6, 20):
        stage4(u)
    for n, src in enumerate((s1, s3, t1, t3)):
        drain(src.at[pl.ds(0, N - 1)], a2s.at[n])
    for n, rcv in enumerate((nrcv, trcv)):
        drain(rcv.at[pl.ds(0, N - 1)], lns.at[n])
    drain(xr_ref, xs.at[0])
    drain(gr_ref, gss.at[0])
    drain(b_ref, p1s.at[0])
    drain(a_ref, p1s.at[1])
    drain(q_ref.at[:, pl.ds(0, 3)], p2s.at[0])
    drain(w_ref.at[:, pl.ds(0, 3)], p3s.at[0])


def results(g_ref, w_ref, gi_ref, oq_ref, ok_ref, ov_ref, save):
    writes = [
        pltpu.make_async_copy(g_ref, gi_ref, save.at[0]),
        pltpu.make_async_copy(w_ref.at[:, pl.ds(0, H * DV)], ov_ref, save.at[1]),
        pltpu.make_async_copy(w_ref.at[:, pl.ds(H * DV, 128)], oq_ref, save.at[2]),
        pltpu.make_async_copy(w_ref.at[:, pl.ds(H * DV + 128, 128)], ok_ref, save.at[3]),
    ]
    for copy in writes:
        copy.start()
    for copy in writes:
        copy.wait()


def body(inputs, cotangent, w_query, w_key, w_value):
    vm = lambda *shape: pltpu.VMEM(shape, F32)
    vb = lambda *shape: pltpu.VMEM(shape, BF)
    sems = lambda *sizes: pltpu.SemaphoreType.DMA(sizes)
    state = lambda: vm(N, PART, DV)
    scratch = [
        vb(T, D), vb(T, H * DV), vb(D, 128), vb(D, 128), vb(D, H * DV),
        vm(H, DK, T), vm(H, DK, T), vb(H, F, T), vb(H, F, T), vb(H, T, F), vb(H, T, F), vb(H, T, DV),
        vb(H, T, T), vb(H, T, T), vm(H, T, DV), vm(H, T, DV), vb(H, T, DV), vb(H, T, DV), vm(H, T, T),
        vm(H, T, DV), vm(H, F, T), vb(H, F, DV), vb(H, F, DV),
        state(), state(), state(), state(), state(), state(), state(), state(),
        vm(10, DV), vm(N, 10, DV), vm(10, DV), vm(N, 10, DV),
        vm(2, N, 16, T), vm(N, 16, T), vb(D // 2, 2 * T), vm(5, T, 256), vm(5, T, 256), vb(2 * T, 1280),
        vm(UNITS, 4, 4, 4, 8, DV), vm(UNITS, 2, 2, 4, 8, DV), vm(UNITS, 2, 4, 4, 8, DV),
        vm(UNITS, 4, 4, 8, DV), vm(UNITS, 4, 4, 8, DV), vm(UNITS, 4, 8, DV), vm(UNITS, 4, 8, DV),
        sems(6), sems(4), sems(4, N), sems(2), sems(2), sems(1), sems(1), sems(1), sems(5),
        sems(2), sems(UNITS, 2), sems(1), sems(UNITS), sems(1), sems(UNITS),
    ]
    grad_in, grad_w = pl.pallas_call(
        kernel,
        out_shape=[vb(T, D), vm(16, 1280)],
        in_specs=[HBM] * 5,
        out_specs=[VMEM] * 2,
        scratch_shapes=scratch,
        compiler_params=pltpu.CompilerParams(
            collective_id=0, has_side_effects=True, vmem_limit_bytes=60 << 20
        ),
    )(inputs[0], cotangent[0], w_query, w_key, w_value)
    grad_in, grad_wq, grad_wk, grad_wv = pl.pallas_call(
        results,
        out_shape=[
            jax.ShapeDtypeStruct((T, D), BF),
            jax.ShapeDtypeStruct((16, 128), F32),
            jax.ShapeDtypeStruct((16, 128), F32),
            jax.ShapeDtypeStruct((16, H * DV), F32),
        ],
        in_specs=[VMEM] * 2,
        out_specs=[HBM] * 4,
        scratch_shapes=[sems(4)],
    )(*(pltpu.with_memory_space_constraint(g, pltpu.VMEM) for g in (grad_in, grad_w)))
    return (grad_in[None], grad_wq, grad_wk, grad_wv)


def solution(mesh):
    in_specs = (P("batch", "seq", None), P("batch", "seq", None), P(), P(), P())
    out_specs = (
        P("batch", "seq", None),
        P(("seq", "batch"), None),
        P(("seq", "batch"), None),
        P(("seq", "batch"), None),
    )
    return jax.shard_map(body, mesh=mesh, in_specs=in_specs, out_specs=out_specs, check_vma=False)
```

```python
import functools
import math

import jax
import jax.numpy as jnp
from jax import lax
from jax.experimental import pallas as pl
from jax.experimental.pallas import tpu as pltpu
from jax.sharding import PartitionSpec as P

H = 8
DK = 16
DV = 128
F = 160
T = 128
N = 64
PART = F // 8
D = 2048
UNITS = 20
LAST = 14
MESH = pl.DeviceIdType.MESH
BF = jnp.bfloat16
F32 = jnp.float32
ROOT = 1.0 / math.sqrt(2.0)
HBM = pl.BlockSpec(memory_space=pl.ANY)
VMEM = pl.BlockSpec(memory_space=pltpu.VMEM)


OFFSETS = sorted(
    ((a, b, c) for a in range(4) for b in range(4) for c in range(4) if a + b + c),
    key=lambda o: -sum(min(v, 4 - v) for v in o),
)


def dot(left, right, dims=(1, 0)):
    return lax.dot_general(left, right, ((dims[:1], dims[1:]), ((), ())), preferred_element_type=F32)


def halves(a):
    high = a.astype(BF)
    return high, (a - high.astype(F32)).astype(BF)


def dot2(pair, right, dims=(1, 0)):
    return dot(pair[0], right, dims) + dot(pair[1], right, dims)


def dot2r(left, pair, dims=(1, 0)):
    return dot(left, pair[0], dims) + dot(left, pair[1], dims)


def dot3(lefts, rights, dims=(1, 0)):
    return (
        dot(lefts[0], rights[0], dims)
        + dot(lefts[0], rights[1], dims)
        + dot(lefts[1], rights[0], dims)
    )


def ahead(a, d):
    return pltpu.roll(a, (8 - d) % 8, 0) if d % 8 else a


def back(a, d):
    return pltpu.roll(a, d, 0) if d % 8 else a


def phi(u):
    row = lax.broadcasted_iota(jnp.int32, (8, T), 0)
    low, high = u[:8], u[8:]
    tiles = []
    for m, fill in ((low, jnp.zeros((8, T), F32)), (high, (row == 4).astype(F32))):
        tiles.append(m * m * ROOT)
        for d in range(1, 4):
            tiles.append(m * ahead(m, d))
        tiles.append(jnp.where(row < 4, m * ahead(m, 4), fill))
    for d in range(8):
        tiles.append(low * ahead(high, d))
    return jnp.concatenate(tiles + [low, high], 0)


def pull(u, grad):
    row = lax.broadcasted_iota(jnp.int32, (8, T), 0)
    low, high = u[:8], u[8:]
    tile = lambda n: grad[8 * n : 8 * n + 8]
    sums = []
    for at, m in ((0, low), (5, high)):
        total = tile(18 + at // 5) + tile(at) * (2.0 * ROOT) * m
        for d in range(1, 5):
            piece = tile(at + d)
            if d == 4:
                piece = jnp.where(row < 4, piece, 0.0)
            total = total + piece * ahead(m, d) + back(piece * m, d)
        sums.append(total)
    for d in range(8):
        piece = tile(10 + d)
        sums[0] = sums[0] + piece * ahead(high, d)
        sums[1] = sums[1] + back(piece * low, d)
    return jnp.concatenate(sums, 0)


def kernel(
    x_hbm, c_hbm, wq_hbm, wk_hbm, wv_hbm, gi_ref, o_ref,
    x_ref, c_ref, wq_ref, wk_ref, wv_ref,
    uq_ref, uk_ref, fqt, fkt, fqn, fkn, v_ref, ath, atl, ni_ref, rd_ref, gnh, gnl, ga_ref,
    gv_ref, gk_ref, sh_ref, gt_ref,
    s1, s2, s3, s4, t1, t2, t3, t4, nsrc, nrcv, tsrc, trcv,
    xt_ref, xr_ref, xp_ref, gs_ref, gr_ref, gp_ref,
    p_ref, a_ref, b_ref, q_ref, r2_ref, w_ref, r3_ref,
    load, a2s, a2r, lns, lnr, xs, xr, gss, grr, p1s, p1r, p2s, p2r, p4s, p4r, r4_ref, p3s, p3r,
):
    me = lax.axis_index("seq")
    core = lax.axis_index("batch")
    other = 1 - core
    at = (me // 16, (me // 4) % 4, me % 4)
    weight = (16, 4, 1)

    def along(d, c):
        return (me + (c - at[d]) * weight[d], core)

    def copy_to(src, dst, send, recv, device):
        return pltpu.make_async_remote_copy(
            src_ref=src, dst_ref=dst, send_sem=send, recv_sem=recv,
            device_id=device, device_id_type=MESH,
        )

    def push(src, dst, send, recv, device):
        copy = copy_to(src, dst, send, recv, device)
        copy.start()
        return copy

    def drain(ref, sem):
        copy_to(ref, ref, sem, sem, (me, other)).wait_send()

    loads = []
    for n, (src, dst) in enumerate(
        ((x_hbm, x_ref), (wk_hbm, wk_ref), (wq_hbm, wq_ref), (wv_hbm, wv_ref), (c_hbm, c_ref))
    ):
        copy = pltpu.make_async_copy(src, dst, load.at[n])
        copy.start()
        loads.append(copy)

    barrier = pltpu.get_barrier_semaphore()

    def greet(k, carry):
        pl.semaphore_signal(barrier, inc=1, device_id=((me + k) % N, core), device_id_type=MESH)
        return carry

    lax.fori_loop(1, N, greet, 0)
    pl.semaphore_signal(barrier, inc=1, device_id=(me, other), device_id_type=MESH)

    def peers():
        part = [[(at[d] + k) % 4 * weight[d] for k in range(4)] for d in range(3)]
        return [part[0][a] + part[1][b] + part[2][c] for a, b, c in OFFSETS]

    def scatter(src, dst, n):
        for peer in peers():
            copy_to(src.at[peer], dst.at[me], a2s.at[n], a2r.at[n], (peer, core)).start()
        dst[me] = src[me]

    def arrive_all(dst, n):
        blocks = dst.at[pl.ds(0, N - 1)]
        copy_to(blocks, blocks, a2s.at[n], a2r.at[n], (me, other)).wait_recv()

    def scan(src, dst, n, reverse):
        arrive_all(src, n)

        def step(i, run):
            for k in range(8):
                j = N - 1 - 8 * i - k if reverse else 8 * i + k
                dst[j] = run
                run = run + src[j]
            return run

        lax.fori_loop(0, N // 8, step, jnp.zeros((PART, DV), F32))

    def put_state(dst, h, value):
        for j in range(8):
            dst[8 * h + j, :16, :] = value[16 * j : 16 * j + 16]
            dst[8 * h + j, 16:, :] = value[128 + 4 * j : 132 + 4 * j]

    def get_state(src, h):
        tiles = [src[8 * h + j, :16, :] for j in range(8)]
        tiles += [src[8 * h + j, 16:, :] for j in range(8)]
        return jnp.concatenate(tiles, 0)

    def gather(src, rcv, n):
        for peer in peers():
            copy_to(src, rcv.at[me], lns.at[n], lnr.at[n], (peer, core)).start()
        rcv[me] = src[...]

    def gathered(rcv, n, low, high):
        blocks = rcv.at[pl.ds(0, N - 1)]
        copy_to(blocks, blocks, lns.at[n], lnr.at[n], (me, other)).wait_recv()

        def step(j, total):
            return total + rcv[j]

        total = lax.fori_loop(low, high, step, jnp.zeros((10, DV), F32))
        rows = []
        for h in range(H):
            at_lane = 32 * (h % 4)
            rest = total[8 + h // 4 : 9 + h // 4, at_lane : at_lane + 32]
            rows.append(jnp.concatenate([total[h : h + 1], rest], 1))
        return jnp.concatenate(rows, 0)

    def turn(rows):
        wide = jnp.concatenate([rows, jnp.zeros((8, 256 - F), F32)], 1)
        return jnp.concatenate([wide, jnp.zeros((T - 8, 256), F32)], 0).T[:F]

    causal = lax.broadcasted_iota(jnp.int32, (T, T), 0) >= lax.broadcasted_iota(jnp.int32, (T, T), 1)
    anti = lax.broadcasted_iota(jnp.int32, (T, T), 0) <= lax.broadcasted_iota(jnp.int32, (T, T), 1)
    lane = lax.broadcasted_iota(jnp.int32, (T, DV), 1)
    ones = jnp.ones((T, DV), BF)
    rows8 = lax.broadcasted_iota(jnp.int32, (8, DV), 0)

    loads[0].wait()
    loads[1].wait()
    x = x_ref[...]
    flat = dot(x, wk_ref[...]).T * 0.5
    norm = jnp.zeros((8, DV), F32)
    one = jnp.ones((8, T), BF)
    for h in range(H):
        u = flat[DK * h : DK * h + DK]
        uk_ref[h] = u
        f = phi(u)
        ft = f.astype(BF)
        fkt[h] = ft
        fkn[h] = f.T.astype(BF)
        norm = jnp.where(rows8 == h, dot(one, ft[:DV], (1, 1)), norm)
    nsrc[:8] = norm
    for i in range(2):
        last = jnp.concatenate([fkt[h, DV:] for h in range(4 * i, 4 * i + 4)], 0)
        nsrc[8 + i : 9 + i] = dot(one, last, (1, 1))[:1]
    pl.semaphore_wait(barrier, N)
    gather(nsrc, nrcv, 0)

    loads[3].wait()
    for m in range(4):
        both = dot(x, wv_ref[:, 256 * m : 256 * m + 256]).astype(BF)
        for i in range(2):
            val = both[:, i * DV : (i + 1) * DV]
            v_ref[2 * m + i] = val
            put_state(s1, 2 * m + i, dot(fkt[2 * m + i], val))
    loads[2].wait()
    flat = dot(x, wq_ref[...]).T * 0.5
    for h in range(H):
        u = flat[DK * h : DK * h + DK]
        uq_ref[h] = u
        f = phi(u)
        fqt[h] = f.astype(BF)
        fqn[h] = f.T.astype(BF)

    def inside(h):
        attn = halves(jnp.where(causal, dot(fqn[h], fkt[h]), 0.0))
        both = dot2(attn, jnp.concatenate([v_ref[h], ones], 1))
        ni_ref[h] = both[:, :DV]
        rd_ref[h] = both[:, DV:]
        turned = halves(jnp.where(anti, dot(fkn[h], fqt[h]), 0.0))
        ath[h] = turned[0]
        atl[h] = turned[1]

    for h in range(H):
        inside(h)
    scatter(s1, s2, 0)
    prefix = gathered(nrcv, 0, 0, me)
    loads[4].wait()

    for h in range(H):
        row = halves(jnp.broadcast_to(prefix[h : h + 1], (DV, F)))
        den = rd_ref[h] + dot2r(fqn[h], row, (1, 1))
        scale = 1.0 / den
        rd_ref[h] = scale
        numer = c_ref[:, h * DV : (h + 1) * DV].astype(F32) * scale
        gn = halves(numer)
        gnh[h] = gn[0]
        gnl[h] = gn[1]
        put_state(t1, h, dot2r(fqt[h], gn))
    scatter(t1, t2, 2)

    for h in range(H):
        gn = (gnh[h], gnl[h])
        gv_ref[h] = dot3((ath[h], atl[h]), gn)
        ga_ref[h] = dot2(gn, v_ref[h], (1, 1))

    scan(s2, s3, 0, False)
    scatter(s3, s4, 1)

    for b in range(D // 128):
        block = x_ref[:, b * 128 : (b + 1) * 128].astype(F32).T
        for i in range(4):
            for half in range(2):
                row = 32 * i + 16 * half
                xt_ref[half, 4 * b + i] = block[row : row + 16]
    swap = push(xt_ref.at[other], xr_ref, xs.at[0], xr.at[0], (me, other))
    xp_ref[:, :T] = xt_ref[core].reshape(D // 2, T).astype(BF)

    scan(t2, t3, 2, True)
    scatter(t3, t4, 3)

    def share(m, value):
        gp_ref[:T, 256 * m : 256 * m + 256] = value
        gs_ref[m] = value.astype(F32)
        return push(gs_ref.at[m], gr_ref.at[m], gss.at[0], grr.at[m], (me, other))

    turned = turn(prefix)
    columns = halves(turned)
    arrive_all(s4, 1)
    down = jnp.zeros((F, DV), F32)
    grads = []
    for h in range(H):
        state = halves(get_state(s4, h))
        gn = (gnh[h], gnl[h])
        num = ni_ref[h] + dot2r(fqn[h], state)
        numer = gn[0].astype(F32) + gn[1].astype(F32)
        denom = -jnp.sum(numer * num, 1, keepdims=True) * rd_ref[h]
        ga = halves(jnp.where(causal, ga_ref[h] + denom, 0.0))
        mine = halves(jnp.where(lane == h, denom, 0.0))
        left = [jnp.concatenate([s, c], 1) for s, c in zip(state, columns)]
        right = [jnp.concatenate([g, m], 1) for g, m in zip(gn, mine)]
        gfq = dot2r(fkt[h], ga, (1, 1)) + dot3(left, right, (1, 1))
        grads.append(pull(uq_ref[h], gfq) * 0.5)
        gk_ref[h] = dot2r(fqt[h], ga)
        down = down + dot2r(fqt[h], mine)
    rows = jnp.concatenate([down, jnp.zeros((256 - F, DV), F32)], 0).T
    tsrc[:8] = rows[:8, :DV]
    for i in range(2):
        tsrc[8 + i : 9 + i] = jnp.concatenate(
            [rows[h : h + 1, DV:F] for h in range(4 * i, 4 * i + 4)], 1
        )
    gather(tsrc, trcv, 1)
    grad_q = jnp.concatenate(grads, 0).T.astype(BF)

    arrive_all(t4, 3)
    shares = []
    for m in range(4):
        pieces = []
        for h in (2 * m, 2 * m + 1):
            state = halves(get_state(t4, h))
            sh_ref[h] = state[0]
            gt_ref[h] = state[1]
            pieces.append((gv_ref[h] + dot2r(fkn[h], state)).astype(BF))
        shares.append(share(m, jnp.concatenate(pieces, 1)))

    swap.wait_recv()
    xp_ref[:, T:] = xr_ref[...].reshape(D // 2, T).astype(BF)

    def multiply(m):
        shares[m].wait_recv()
        gp_ref[T:, 256 * m : 256 * m + 256] = gr_ref[m].astype(BF)
        right = gp_ref[:, 256 * m : 256 * m + 256]
        for z in range(4):
            part = dot(xp_ref[256 * z : 256 * z + 256, :], right)
            for i in range(2):
                block = part[:, i * DV : (i + 1) * DV].reshape(4, 4, 2, 8, DV)
                for r in range(2):
                    p_ref[4 * m + 2 * i + r, z] = block[:, :, r]

    def line_part(u, g, c, half):
        take = pl.ds(2 * half, 2)
        if g == 0:
            return (u, c, take)
        if g == 1:
            return (u, take, c)
        return (u, take, slice(None), c)

    def arrived(ref, sem, u, more=()):
        if u % 2 == 0:
            pair = ref.at[(pl.ds(u, 2),) + more]
            copy_to(pair, pair, sem, sem, (me, other)).wait_recv()

    def stage0(u):
        g = u % 3
        i = at[g]
        right, left, far = (i + 1) % 4, (i + 3) % 4, (i + 2) % 4
        keys = (
            (far, 0, right, a_ref.at[u, 0]),
            (far, 1, left, a_ref.at[u, 1]),
            (right, 1, right, b_ref.at[u, 0, pl.ds(2, 2)]),
            (left, 0, left, b_ref.at[u, 1, pl.ds(0, 2)]),
        )
        for n, (c, half, peer, dst) in enumerate(keys):
            push(p_ref.at[line_part(u, g, c, half)], dst, p1s.at[0], p1r.at[u // 2, n // 2], along(g, peer))

    def stage1(u):
        g = u % 3
        i = at[g]
        right, left = (i + 1) % 4, (i + 3) % 4
        arrived(a_ref, p1r.at[u // 2, 0], u)
        for n, (peer, half) in enumerate(((right, 0), (left, 1))):
            where = line_part(u, g, peer, half)
            p_ref[where] = p_ref[where] + a_ref[u, n]
            dst = b_ref.at[u, n, pl.ds(2 * half, 2)]
            push(p_ref.at[where], dst, p1s.at[1], p1r.at[u // 2, 1], along(g, peer))

    order = ((1, 2), (2, 0), (0, 1))

    def stage2(u):
        g = u % 3
        arrived(b_ref, p1r.at[u // 2, 1], u)
        for half in range(2):
            mine = p_ref[line_part(u, g, at[g], half)]
            mine = mine + b_ref[u, 0, 2 * half : 2 * half + 2] + b_ref[u, 1, 2 * half : 2 * half + 2]
            for i in range(2):
                if g == 1:
                    q_ref[u, :, 2 * half + i] = mine[i]
                else:
                    q_ref[u, 2 * half + i] = mine[i]
        d, e = order[g]
        if u >= LAST:
            for k in range(1, 16):
                a, b = (at[d] + k // 4) % 4, (at[e] + k % 4) % 4
                peer = me + (a - at[d]) * weight[d] + (b - at[e]) * weight[e]
                dst = r4_ref.at[u - LAST, 4 * at[d] + at[e]]
                push(q_ref.at[u, a, b], dst, p4s.at[0], p4r.at[u // 2 - LAST // 2], (peer, core))
            return
        for k in range(1, 4):
            c = (at[d] + k) % 4
            push(q_ref.at[u, c], r2_ref.at[u, at[d]], p2s.at[0], p2r.at[u // 2], along(d, c))

    def from_line(d, src, dst, recv, u):
        arrived(dst, recv.at[u // 2], u, (pl.ds(0, 3),))
        total = src[u, at[d]]
        for k in range(1, 4):
            total = total + dst[u, (at[d] + k) % 4]
        return total

    def stage3(u):
        if u >= LAST:
            return
        d, e = order[u % 3]
        w_ref[u] = from_line(d, q_ref, r2_ref, p2r, u)
        for k in range(1, 4):
            c = (at[e] + k) % 4
            push(w_ref.at[u, c], r3_ref.at[u, at[e]], p3s.at[0], p3r.at[u // 2], along(e, c))

    def stage4(u):
        if u < LAST:
            total = from_line(order[u % 3][1], w_ref, r3_ref, p3r, u)
        else:
            n = u - LAST
            arrived(r4_ref, p4r.at[n // 2], n, (pl.ds(0, 15),))
            d, e = order[u % 3]
            r4_ref[n, 4 * at[d] + at[e]] = q_ref[u, at[d], at[e]]
            total = r4_ref[n, 0]
            for k in range(1, 16):
                total = total + r4_ref[n, k]
        piece, r = u // 2, u % 2
        rows = slice(8 * r, 8 * r + 8)
        o_ref[rows, piece * DV : (piece + 1) * DV] = total

    for m in range(2):
        multiply(m)
        for u in range(4 * m, 4 * m + 4):
            stage0(u)
    suffix = gathered(trcv, 1, me + 1, N)
    turned = turn(suffix)
    grads = []
    for h in range(H):
        gfk = gk_ref[h] + dot2((sh_ref[h], gt_ref[h]), v_ref[h], (1, 1)) + turned[:, h : h + 1]
        grads.append(pull(uk_ref[h], gfk) * 0.5)
    grad_k = jnp.concatenate(grads, 0).T.astype(BF)
    shares.append(share(4, jnp.concatenate([grad_q, grad_k], 1)))
    for m in range(2, 5):
        multiply(m)
        for u in range(4 * m, 4 * m + 4):
            stage0(u)
    wide = D // 8

    def inputs(n):
        cut = slice(n * wide, (n + 1) * wide)
        total = dot(gp_ref[:T, : H * DV], wv_ref[cut, :], (1, 1))
        total = total + dot(gp_ref[:T, H * DV : H * DV + 128], wq_ref[cut, :], (1, 1))
        total = total + dot(gp_ref[:T, H * DV + 128 :], wk_ref[cut, :], (1, 1))
        gi_ref[:, cut] = total.astype(BF)

    for n in range(4):
        inputs(n)
    for u in range(8):
        stage1(u)
    for n in range(4, 8):
        inputs(n)
    for u in range(8, 20):
        stage1(u)
        if u >= 14:
            stage2(u - 14)
    for u in range(6, 20):
        stage2(u)
        if u >= 12:
            stage3(u - 12)
    for u in range(8, 20):
        stage3(u)
        if u >= 14:
            stage4(u - 14)
    for u in range(6, 20):
        stage4(u)
    for n, src in enumerate((s1, s3, t1, t3)):
        drain(src.at[pl.ds(0, N - 1)], a2s.at[n])
    for n, rcv in enumerate((nrcv, trcv)):
        drain(rcv.at[pl.ds(0, N - 1)], lns.at[n])
    drain(xr_ref, xs.at[0])
    drain(gr_ref, gss.at[0])
    drain(b_ref, p1s.at[0])
    drain(a_ref, p1s.at[1])
    drain(q_ref.at[pl.ds(0, LAST), pl.ds(0, 3)], p2s.at[0])
    drain(w_ref.at[pl.ds(0, LAST), pl.ds(0, 3)], p3s.at[0])
    drain(r4_ref.at[:, pl.ds(0, 15)], p4s.at[0])


def results(g_ref, w_ref, gi_ref, oq_ref, ok_ref, ov_ref, save):
    writes = [
        pltpu.make_async_copy(g_ref, gi_ref, save.at[0]),
        pltpu.make_async_copy(w_ref.at[:, pl.ds(0, H * DV)], ov_ref, save.at[1]),
        pltpu.make_async_copy(w_ref.at[:, pl.ds(H * DV, 128)], oq_ref, save.at[2]),
        pltpu.make_async_copy(w_ref.at[:, pl.ds(H * DV + 128, 128)], ok_ref, save.at[3]),
    ]
    for copy in writes:
        copy.start()
    for copy in writes:
        copy.wait()


def body(inputs, cotangent, w_query, w_key, w_value):
    vm = lambda *shape: pltpu.VMEM(shape, F32)
    vb = lambda *shape: pltpu.VMEM(shape, BF)
    sems = lambda *sizes: pltpu.SemaphoreType.DMA(sizes)
    state = lambda: vm(N, PART, DV)
    scratch = [
        vb(T, D), vb(T, H * DV), vb(D, 128), vb(D, 128), vb(D, H * DV),
        vm(H, DK, T), vm(H, DK, T), vb(H, F, T), vb(H, F, T), vb(H, T, F), vb(H, T, F), vb(H, T, DV),
        vb(H, T, T), vb(H, T, T), vm(H, T, DV), vm(H, T, DV), vb(H, T, DV), vb(H, T, DV), vm(H, T, T),
        vm(H, T, DV), vm(H, F, T), vb(H, F, DV), vb(H, F, DV),
        state(), state(), state(), state(), state(), state(), state(), state(),
        vm(10, DV), vm(N, 10, DV), vm(10, DV), vm(N, 10, DV),
        vm(2, N, 16, T), vm(N, 16, T), vb(D // 2, 2 * T), vm(5, T, 256), vm(5, T, 256), vb(2 * T, 1280),
        vm(UNITS, 4, 4, 4, 8, DV), vm(UNITS, 2, 2, 4, 8, DV), vm(UNITS, 2, 4, 4, 8, DV),
        vm(UNITS, 4, 4, 8, DV), vm(UNITS, 4, 4, 8, DV), vm(UNITS, 4, 8, DV), vm(UNITS, 4, 8, DV),
        sems(5), sems(4), sems(4), sems(2), sems(2), sems(1), sems(1), sems(1), sems(5),
        sems(2), sems(UNITS // 2, 2), sems(1), sems(UNITS // 2), sems(1), sems(3), vm(UNITS - LAST, 16, 8, DV), sems(1), sems(UNITS // 2),
    ]
    grad_in, grad_w = pl.pallas_call(
        kernel,
        out_shape=[vb(T, D), vm(16, 1280)],
        in_specs=[HBM] * 5,
        out_specs=[VMEM] * 2,
        scratch_shapes=scratch,
        compiler_params=pltpu.CompilerParams(
            collective_id=0, has_side_effects=True, vmem_limit_bytes=60 << 20
        ),
    )(inputs[0], cotangent[0], w_query, w_key, w_value)
    grad_in, grad_wq, grad_wk, grad_wv = pl.pallas_call(
        results,
        out_shape=[
            jax.ShapeDtypeStruct((T, D), BF),
            jax.ShapeDtypeStruct((16, 128), F32),
            jax.ShapeDtypeStruct((16, 128), F32),
            jax.ShapeDtypeStruct((16, H * DV), F32),
        ],
        in_specs=[VMEM] * 2,
        out_specs=[HBM] * 4,
        scratch_shapes=[sems(4)],
    )(*(pltpu.with_memory_space_constraint(g, pltpu.VMEM) for g in (grad_in, grad_w)))
    return (grad_in[None], grad_wq, grad_wk, grad_wv)


def solution(mesh):
    in_specs = (P("batch", "seq", None), P("batch", "seq", None), P(), P(), P())
    out_specs = (
        P("batch", "seq", None),
        P(("seq", "batch"), None),
        P(("seq", "batch"), None),
        P(("seq", "batch"), None),
    )
    return jax.shard_map(body, mesh=mesh, in_specs=in_specs, out_specs=out_specs, check_vma=False)
```

```python
import functools
import math

import jax
import jax.numpy as jnp
from jax import lax
from jax.experimental import pallas as pl
from jax.experimental.pallas import tpu as pltpu
from jax.sharding import PartitionSpec as P

H = 8
DK = 16
DV = 128
F = 160
T = 128
N = 64
PART = F // 8
D = 2048
UNITS = 20
LAST = 14
MESH = pl.DeviceIdType.MESH
BF = jnp.bfloat16
F32 = jnp.float32
ROOT = 1.0 / math.sqrt(2.0)
HBM = pl.BlockSpec(memory_space=pl.ANY)
VMEM = pl.BlockSpec(memory_space=pltpu.VMEM)


OFFSETS = sorted(
    ((a, b, c) for a in range(4) for b in range(4) for c in range(4) if a + b + c),
    key=lambda o: -sum(min(v, 4 - v) for v in o),
)


def dot(left, right, dims=(1, 0)):
    return lax.dot_general(left, right, ((dims[:1], dims[1:]), ((), ())), preferred_element_type=F32)


def halves(a):
    high = a.astype(BF)
    return high, (a - high.astype(F32)).astype(BF)


def dot2(pair, right, dims=(1, 0)):
    return dot(pair[0], right, dims) + dot(pair[1], right, dims)


def dot2r(left, pair, dims=(1, 0)):
    return dot(left, pair[0], dims) + dot(left, pair[1], dims)


def dot3(lefts, rights, dims=(1, 0)):
    return (
        dot(lefts[0], rights[0], dims)
        + dot(lefts[0], rights[1], dims)
        + dot(lefts[1], rights[0], dims)
    )


def ahead(a, d):
    return pltpu.roll(a, (8 - d) % 8, 0) if d % 8 else a


def back(a, d):
    return pltpu.roll(a, d, 0) if d % 8 else a


def phi(u):
    row = lax.broadcasted_iota(jnp.int32, (8, T), 0)
    low, high = u[:8], u[8:]
    tiles = []
    for m, fill in ((low, jnp.zeros((8, T), F32)), (high, (row == 4).astype(F32))):
        tiles.append(m * m * ROOT)
        for d in range(1, 4):
            tiles.append(m * ahead(m, d))
        tiles.append(jnp.where(row < 4, m * ahead(m, 4), fill))
    for d in range(8):
        tiles.append(low * ahead(high, d))
    return jnp.concatenate(tiles + [low, high], 0)


def pull(u, grad):
    row = lax.broadcasted_iota(jnp.int32, (8, T), 0)
    low, high = u[:8], u[8:]
    tile = lambda n: grad[8 * n : 8 * n + 8]
    sums = []
    for at, m in ((0, low), (5, high)):
        total = tile(18 + at // 5) + tile(at) * (2.0 * ROOT) * m
        for d in range(1, 5):
            piece = tile(at + d)
            if d == 4:
                piece = jnp.where(row < 4, piece, 0.0)
            total = total + piece * ahead(m, d) + back(piece * m, d)
        sums.append(total)
    for d in range(8):
        piece = tile(10 + d)
        sums[0] = sums[0] + piece * ahead(high, d)
        sums[1] = sums[1] + back(piece * low, d)
    return jnp.concatenate(sums, 0)


def kernel(
    x_hbm, c_hbm, wq_hbm, wk_hbm, wv_hbm, gi_ref, o_ref,
    x_ref, c_ref, wq_ref, wk_ref, wv_ref,
    uq_ref, uk_ref, fqt, fkt, fqn, fkn, v_ref, ath, atl, ni_ref, rd_ref, gnh, gnl, ga_ref,
    gv_ref, gk_ref, sh_ref, gt_ref,
    s1, s2, s3, s4, t1, t2, t3, t4, nsrc, nrcv, tsrc, trcv,
    xt_ref, xr_ref, xp_ref, gs_ref, gr_ref, gp_ref,
    p_ref, a_ref, b_ref, q_ref, r2_ref, w_ref, r3_ref,
    load, a2s, a2r, lns, lnr, xs, xr, gss, grr, p1s, p1r, p2s, p2r, p4s, p4r, r4_ref, p3s, p3r,
):
    me = lax.axis_index("seq")
    core = lax.axis_index("batch")
    other = 1 - core
    at = (me // 16, (me // 4) % 4, me % 4)
    weight = (16, 4, 1)

    def along(d, c):
        return (me + (c - at[d]) * weight[d], core)

    def copy_to(src, dst, send, recv, device):
        return pltpu.make_async_remote_copy(
            src_ref=src, dst_ref=dst, send_sem=send, recv_sem=recv,
            device_id=device, device_id_type=MESH,
        )

    def push(src, dst, send, recv, device):
        copy = copy_to(src, dst, send, recv, device)
        copy.start()
        return copy

    def drain(ref, sem):
        copy_to(ref, ref, sem, sem, (me, other)).wait_send()

    def peers():
        part = [[(at[d] + k) % 4 * weight[d] for k in range(4)] for d in range(3)]
        return [part[0][a] + part[1][b] + part[2][c] for a, b, c in OFFSETS]

    barrier = pltpu.get_barrier_semaphore()
    for peer in peers():
        pl.semaphore_signal(barrier, inc=1, device_id=(peer, core), device_id_type=MESH)
    pl.semaphore_signal(barrier, inc=1, device_id=(me, other), device_id_type=MESH)

    loads = []
    for n, (src, dst) in enumerate(
        ((x_hbm, x_ref), (wk_hbm, wk_ref), (wq_hbm, wq_ref), (wv_hbm, wv_ref), (c_hbm, c_ref))
    ):
        copy = pltpu.make_async_copy(src, dst, load.at[n])
        copy.start()
        loads.append(copy)

    def scatter(src, dst, n):
        for peer in peers():
            copy_to(src.at[peer], dst.at[me], a2s.at[n], a2r.at[n], (peer, core)).start()
        dst[me] = src[me]

    def arrive_all(dst, n):
        blocks = dst.at[pl.ds(0, N - 1)]
        copy_to(blocks, blocks, a2s.at[n], a2r.at[n], (me, other)).wait_recv()

    def scan(src, dst, n, reverse):
        arrive_all(src, n)

        def step(i, run):
            for k in range(8):
                j = N - 1 - 8 * i - k if reverse else 8 * i + k
                dst[j] = run
                run = run + src[j]
            return run

        lax.fori_loop(0, N // 8, step, jnp.zeros((PART, DV), F32))

    def put_state(dst, h, value):
        for j in range(8):
            dst[8 * h + j, :16, :] = value[16 * j : 16 * j + 16]
            dst[8 * h + j, 16:, :] = value[128 + 4 * j : 132 + 4 * j]

    def get_state(src, h):
        tiles = [src[8 * h + j, :16, :] for j in range(8)]
        tiles += [src[8 * h + j, 16:, :] for j in range(8)]
        return jnp.concatenate(tiles, 0)

    def gather(src, rcv, n):
        for peer in peers():
            copy_to(src, rcv.at[me], lns.at[n], lnr.at[n], (peer, core)).start()
        rcv[me] = src[...]

    def gathered(rcv, n, low, high):
        blocks = rcv.at[pl.ds(0, N - 1)]
        copy_to(blocks, blocks, lns.at[n], lnr.at[n], (me, other)).wait_recv()

        def step(j, total):
            return total + rcv[j]

        total = lax.fori_loop(low, high, step, jnp.zeros((10, DV), F32))
        rows = []
        for h in range(H):
            at_lane = 32 * (h % 4)
            rest = total[8 + h // 4 : 9 + h // 4, at_lane : at_lane + 32]
            rows.append(jnp.concatenate([total[h : h + 1], rest], 1))
        return jnp.concatenate(rows, 0)

    def turn(rows):
        wide = jnp.concatenate([rows, jnp.zeros((8, 256 - F), F32)], 1)
        return jnp.concatenate([wide, jnp.zeros((T - 8, 256), F32)], 0).T[:F]

    causal = lax.broadcasted_iota(jnp.int32, (T, T), 0) >= lax.broadcasted_iota(jnp.int32, (T, T), 1)
    anti = lax.broadcasted_iota(jnp.int32, (T, T), 0) <= lax.broadcasted_iota(jnp.int32, (T, T), 1)
    lane = lax.broadcasted_iota(jnp.int32, (T, DV), 1)
    ones = jnp.ones((T, DV), BF)
    rows8 = lax.broadcasted_iota(jnp.int32, (8, DV), 0)

    loads[0].wait()
    loads[1].wait()
    x = x_ref[...]
    flat = dot(x, wk_ref[...]).T * 0.5
    norm = jnp.zeros((8, DV), F32)
    one = jnp.ones((8, T), BF)
    for h in range(H):
        u = flat[DK * h : DK * h + DK]
        uk_ref[h] = u
        f = phi(u)
        ft = f.astype(BF)
        fkt[h] = ft
        fkn[h] = f.T.astype(BF)
        norm = jnp.where(rows8 == h, dot(one, ft[:DV], (1, 1)), norm)
    nsrc[:8] = norm
    for i in range(2):
        last = jnp.concatenate([fkt[h, DV:] for h in range(4 * i, 4 * i + 4)], 0)
        nsrc[8 + i : 9 + i] = dot(one, last, (1, 1))[:1]
    pl.semaphore_wait(barrier, N)
    gather(nsrc, nrcv, 0)

    loads[3].wait()
    for m in range(4):
        both = dot(x, wv_ref[:, 256 * m : 256 * m + 256]).astype(BF)
        for i in range(2):
            val = both[:, i * DV : (i + 1) * DV]
            v_ref[2 * m + i] = val
            put_state(s1, 2 * m + i, dot(fkt[2 * m + i], val))
    loads[2].wait()
    flat = dot(x, wq_ref[...]).T * 0.5
    for h in range(H):
        u = flat[DK * h : DK * h + DK]
        uq_ref[h] = u
        f = phi(u)
        fqt[h] = f.astype(BF)
        fqn[h] = f.T.astype(BF)

    def inside(h):
        attn = halves(jnp.where(causal, dot(fqn[h], fkt[h]), 0.0))
        both = dot2(attn, jnp.concatenate([v_ref[h], ones], 1))
        ni_ref[h] = both[:, :DV]
        rd_ref[h] = both[:, DV:]
        turned = halves(jnp.where(anti, dot(fkn[h], fqt[h]), 0.0))
        ath[h] = turned[0]
        atl[h] = turned[1]

    for h in range(H):
        inside(h)
    scatter(s1, s2, 0)
    prefix = gathered(nrcv, 0, 0, me)
    loads[4].wait()

    for h in range(H):
        row = halves(jnp.broadcast_to(prefix[h : h + 1], (DV, F)))
        den = rd_ref[h] + dot2r(fqn[h], row, (1, 1))
        scale = 1.0 / den
        rd_ref[h] = scale
        numer = c_ref[:, h * DV : (h + 1) * DV].astype(F32) * scale
        gn = halves(numer)
        gnh[h] = gn[0]
        gnl[h] = gn[1]
        put_state(t1, h, dot2r(fqt[h], gn))
    scatter(t1, t2, 2)

    for h in range(H):
        gn = (gnh[h], gnl[h])
        gv_ref[h] = dot3((ath[h], atl[h]), gn)
        ga_ref[h] = dot2(gn, v_ref[h], (1, 1))

    scan(s2, s3, 0, False)
    scatter(s3, s4, 1)

    for b in range(D // 128):
        block = x_ref[:, b * 128 : (b + 1) * 128].astype(F32).T
        for i in range(4):
            for half in range(2):
                row = 32 * i + 16 * half
                xt_ref[half, 4 * b + i] = block[row : row + 16]
    swap = push(xt_ref.at[other], xr_ref, xs.at[0], xr.at[0], (me, other))
    xp_ref[:, :T] = xt_ref[core].reshape(D // 2, T).astype(BF)

    scan(t2, t3, 2, True)
    scatter(t3, t4, 3)

    def share(m, value):
        gp_ref[:T, 256 * m : 256 * m + 256] = value
        gs_ref[m] = value.astype(F32)
        return push(gs_ref.at[m], gr_ref.at[m], gss.at[0], grr.at[m], (me, other))

    turned = turn(prefix)
    columns = halves(turned)
    arrive_all(s4, 1)
    down = jnp.zeros((F, DV), F32)
    grads = []
    for h in range(H):
        state = halves(get_state(s4, h))
        gn = (gnh[h], gnl[h])
        num = ni_ref[h] + dot2r(fqn[h], state)
        numer = gn[0].astype(F32) + gn[1].astype(F32)
        denom = -jnp.sum(numer * num, 1, keepdims=True) * rd_ref[h]
        ga = halves(jnp.where(causal, ga_ref[h] + denom, 0.0))
        mine = halves(jnp.where(lane == h, denom, 0.0))
        left = [jnp.concatenate([s, c], 1) for s, c in zip(state, columns)]
        right = [jnp.concatenate([g, m], 1) for g, m in zip(gn, mine)]
        gfq = dot2r(fkt[h], ga, (1, 1)) + dot3(left, right, (1, 1))
        grads.append(pull(uq_ref[h], gfq) * 0.5)
        gk_ref[h] = dot2r(fqt[h], ga)
        down = down + dot2r(fqt[h], mine)
    rows = jnp.concatenate([down, jnp.zeros((256 - F, DV), F32)], 0).T
    tsrc[:8] = rows[:8, :DV]
    for i in range(2):
        tsrc[8 + i : 9 + i] = jnp.concatenate(
            [rows[h : h + 1, DV:F] for h in range(4 * i, 4 * i + 4)], 1
        )
    gather(tsrc, trcv, 1)
    grad_q = jnp.concatenate(grads, 0).T.astype(BF)

    arrive_all(t4, 3)
    shares = []
    for m in range(4):
        pieces = []
        for h in (2 * m, 2 * m + 1):
            state = halves(get_state(t4, h))
            sh_ref[h] = state[0]
            gt_ref[h] = state[1]
            pieces.append((gv_ref[h] + dot2r(fkn[h], state)).astype(BF))
        shares.append(share(m, jnp.concatenate(pieces, 1)))

    swap.wait_recv()
    xp_ref[:, T:] = xr_ref[...].reshape(D // 2, T).astype(BF)

    def multiply(m):
        shares[m].wait_recv()
        gp_ref[T:, 256 * m : 256 * m + 256] = gr_ref[m].astype(BF)
        right = gp_ref[:, 256 * m : 256 * m + 256]
        for z in range(4):
            part = dot(xp_ref[256 * z : 256 * z + 256, :], right)
            for i in range(2):
                block = part[:, i * DV : (i + 1) * DV].reshape(4, 4, 2, 8, DV)
                for r in range(2):
                    p_ref[4 * m + 2 * i + r, z] = block[:, :, r]

    def line_part(u, g, c, half):
        take = pl.ds(2 * half, 2)
        if g == 0:
            return (u, c, take)
        if g == 1:
            return (u, take, c)
        return (u, take, slice(None), c)

    def arrived(ref, sem, u, more=()):
        if u % 2 == 0:
            pair = ref.at[(pl.ds(u, 2),) + more]
            copy_to(pair, pair, sem, sem, (me, other)).wait_recv()

    def stage0(u):
        g = u % 3
        i = at[g]
        right, left, far = (i + 1) % 4, (i + 3) % 4, (i + 2) % 4
        keys = (
            (far, 0, right, a_ref.at[u, 0]),
            (far, 1, left, a_ref.at[u, 1]),
            (right, 1, right, b_ref.at[u, 0, pl.ds(2, 2)]),
            (left, 0, left, b_ref.at[u, 1, pl.ds(0, 2)]),
        )
        for n, (c, half, peer, dst) in enumerate(keys):
            push(p_ref.at[line_part(u, g, c, half)], dst, p1s.at[0], p1r.at[u // 2, n // 2], along(g, peer))

    def stage1(u):
        g = u % 3
        i = at[g]
        right, left = (i + 1) % 4, (i + 3) % 4
        arrived(a_ref, p1r.at[u // 2, 0], u)
        for n, (peer, half) in enumerate(((right, 0), (left, 1))):
            where = line_part(u, g, peer, half)
            p_ref[where] = p_ref[where] + a_ref[u, n]
            dst = b_ref.at[u, n, pl.ds(2 * half, 2)]
            push(p_ref.at[where], dst, p1s.at[1], p1r.at[u // 2, 1], along(g, peer))

    order = ((1, 2), (2, 0), (0, 1))

    def stage2(u):
        g = u % 3
        arrived(b_ref, p1r.at[u // 2, 1], u)
        for half in range(2):
            mine = p_ref[line_part(u, g, at[g], half)]
            mine = mine + b_ref[u, 0, 2 * half : 2 * half + 2] + b_ref[u, 1, 2 * half : 2 * half + 2]
            for i in range(2):
                if g == 1:
                    q_ref[u, :, 2 * half + i] = mine[i]
                else:
                    q_ref[u, 2 * half + i] = mine[i]
        d, e = order[g]
        if u >= LAST:
            for k in range(1, 16):
                a, b = (at[d] + k // 4) % 4, (at[e] + k % 4) % 4
                peer = me + (a - at[d]) * weight[d] + (b - at[e]) * weight[e]
                dst = r4_ref.at[u - LAST, 4 * at[d] + at[e]]
                push(q_ref.at[u, a, b], dst, p4s.at[0], p4r.at[u // 2 - LAST // 2], (peer, core))
            return
        for k in range(1, 4):
            c = (at[d] + k) % 4
            push(q_ref.at[u, c], r2_ref.at[u, at[d]], p2s.at[0], p2r.at[u // 2], along(d, c))

    def from_line(d, src, dst, recv, u):
        arrived(dst, recv.at[u // 2], u, (pl.ds(0, 3),))
        total = src[u, at[d]]
        for k in range(1, 4):
            total = total + dst[u, (at[d] + k) % 4]
        return total

    def stage3(u):
        if u >= LAST:
            return
        d, e = order[u % 3]
        w_ref[u] = from_line(d, q_ref, r2_ref, p2r, u)
        for k in range(1, 4):
            c = (at[e] + k) % 4
            push(w_ref.at[u, c], r3_ref.at[u, at[e]], p3s.at[0], p3r.at[u // 2], along(e, c))

    def stage4(u):
        if u < LAST:
            total = from_line(order[u % 3][1], w_ref, r3_ref, p3r, u)
        else:
            n = u - LAST
            arrived(r4_ref, p4r.at[n // 2], n, (pl.ds(0, 15),))
            d, e = order[u % 3]
            r4_ref[n, 4 * at[d] + at[e]] = q_ref[u, at[d], at[e]]
            total = r4_ref[n, 0]
            for k in range(1, 16):
                total = total + r4_ref[n, k]
        piece, r = u // 2, u % 2
        rows = slice(8 * r, 8 * r + 8)
        o_ref[rows, piece * DV : (piece + 1) * DV] = total

    for m in range(4):
        multiply(m)
        for u in range(4 * m, 4 * m + 4):
            stage0(u)
    for u in range(4):
        stage1(u)
    suffix = gathered(trcv, 1, me + 1, N)
    turned = turn(suffix)
    grads = []
    for h in range(H):
        gfk = gk_ref[h] + dot2((sh_ref[h], gt_ref[h]), v_ref[h], (1, 1)) + turned[:, h : h + 1]
        grads.append(pull(uk_ref[h], gfk) * 0.5)
    grad_k = jnp.concatenate(grads, 0).T.astype(BF)
    shares.append(share(4, jnp.concatenate([grad_q, grad_k], 1)))
    for m in range(4, 5):
        multiply(m)
        for u in range(4 * m, 4 * m + 4):
            stage0(u)
    wide = D // 8

    def inputs(n):
        cut = slice(n * wide, (n + 1) * wide)
        total = dot(gp_ref[:T, : H * DV], wv_ref[cut, :], (1, 1))
        total = total + dot(gp_ref[:T, H * DV : H * DV + 128], wq_ref[cut, :], (1, 1))
        total = total + dot(gp_ref[:T, H * DV + 128 :], wk_ref[cut, :], (1, 1))
        gi_ref[:, cut] = total.astype(BF)

    for n in range(4):
        inputs(n)
    for u in range(4, 8):
        stage1(u)
    for n in range(4, 8):
        inputs(n)
    for u in range(8, 20):
        stage1(u)
        if u >= 14:
            stage2(u - 14)
    for u in range(6, 20):
        stage2(u)
        if u >= 12:
            stage3(u - 12)
    for u in range(8, 20):
        stage3(u)
        if u >= 14:
            stage4(u - 14)
    for u in range(6, 20):
        stage4(u)
    for n, src in enumerate((s1, s3, t1, t3)):
        drain(src.at[pl.ds(0, N - 1)], a2s.at[n])
    for n, rcv in enumerate((nrcv, trcv)):
        drain(rcv.at[pl.ds(0, N - 1)], lns.at[n])
    drain(xr_ref, xs.at[0])
    drain(gr_ref, gss.at[0])
    drain(b_ref, p1s.at[0])
    drain(a_ref, p1s.at[1])
    drain(q_ref.at[pl.ds(0, LAST), pl.ds(0, 3)], p2s.at[0])
    drain(w_ref.at[pl.ds(0, LAST), pl.ds(0, 3)], p3s.at[0])
    drain(r4_ref.at[:, pl.ds(0, 15)], p4s.at[0])


def results(g_ref, w_ref, gi_ref, oq_ref, ok_ref, ov_ref, save):
    writes = [
        pltpu.make_async_copy(g_ref, gi_ref, save.at[0]),
        pltpu.make_async_copy(w_ref.at[:, pl.ds(0, H * DV)], ov_ref, save.at[1]),
        pltpu.make_async_copy(w_ref.at[:, pl.ds(H * DV, 128)], oq_ref, save.at[2]),
        pltpu.make_async_copy(w_ref.at[:, pl.ds(H * DV + 128, 128)], ok_ref, save.at[3]),
    ]
    for copy in writes:
        copy.start()
    for copy in writes:
        copy.wait()


def body(inputs, cotangent, w_query, w_key, w_value):
    vm = lambda *shape: pltpu.VMEM(shape, F32)
    vb = lambda *shape: pltpu.VMEM(shape, BF)
    sems = lambda *sizes: pltpu.SemaphoreType.DMA(sizes)
    state = lambda: vm(N, PART, DV)
    scratch = [
        vb(T, D), vb(T, H * DV), vb(D, 128), vb(D, 128), vb(D, H * DV),
        vm(H, DK, T), vm(H, DK, T), vb(H, F, T), vb(H, F, T), vb(H, T, F), vb(H, T, F), vb(H, T, DV),
        vb(H, T, T), vb(H, T, T), vm(H, T, DV), vm(H, T, DV), vb(H, T, DV), vb(H, T, DV), vm(H, T, T),
        vm(H, T, DV), vm(H, F, T), vb(H, F, DV), vb(H, F, DV),
        state(), state(), state(), state(), state(), state(), state(), state(),
        vm(10, DV), vm(N, 10, DV), vm(10, DV), vm(N, 10, DV),
        vm(2, N, 16, T), vm(N, 16, T), vb(D // 2, 2 * T), vm(5, T, 256), vm(5, T, 256), vb(2 * T, 1280),
        vm(UNITS, 4, 4, 4, 8, DV), vm(UNITS, 2, 2, 4, 8, DV), vm(UNITS, 2, 4, 4, 8, DV),
        vm(UNITS, 4, 4, 8, DV), vm(UNITS, 4, 4, 8, DV), vm(UNITS, 4, 8, DV), vm(UNITS, 4, 8, DV),
        sems(5), sems(4), sems(4), sems(2), sems(2), sems(1), sems(1), sems(1), sems(5),
        sems(2), sems(UNITS // 2, 2), sems(1), sems(UNITS // 2), sems(1), sems(3), vm(UNITS - LAST, 16, 8, DV), sems(1), sems(UNITS // 2),
    ]
    grad_in, grad_w = pl.pallas_call(
        kernel,
        out_shape=[vb(T, D), vm(16, 1280)],
        in_specs=[HBM] * 5,
        out_specs=[VMEM] * 2,
        scratch_shapes=scratch,
        compiler_params=pltpu.CompilerParams(
            collective_id=0, has_side_effects=True, vmem_limit_bytes=60 << 20
        ),
    )(inputs[0], cotangent[0], w_query, w_key, w_value)
    grad_in, grad_wq, grad_wk, grad_wv = pl.pallas_call(
        results,
        out_shape=[
            jax.ShapeDtypeStruct((T, D), BF),
            jax.ShapeDtypeStruct((16, 128), F32),
            jax.ShapeDtypeStruct((16, 128), F32),
            jax.ShapeDtypeStruct((16, H * DV), F32),
        ],
        in_specs=[VMEM] * 2,
        out_specs=[HBM] * 4,
        scratch_shapes=[sems(4)],
    )(*(pltpu.with_memory_space_constraint(g, pltpu.VMEM) for g in (grad_in, grad_w)))
    return (grad_in[None], grad_wq, grad_wk, grad_wv)


def solution(mesh):
    in_specs = (P("batch", "seq", None), P("batch", "seq", None), P(), P(), P())
    out_specs = (
        P("batch", "seq", None),
        P(("seq", "batch"), None),
        P(("seq", "batch"), None),
        P(("seq", "batch"), None),
    )
    return jax.shard_map(body, mesh=mesh, in_specs=in_specs, out_specs=out_specs, check_vma=False)
```

```python
import functools
import math

import jax
import jax.numpy as jnp
from jax import lax
from jax.experimental import pallas as pl
from jax.experimental.pallas import tpu as pltpu
from jax.sharding import PartitionSpec as P

H = 8
DK = 16
DV = 128
F = 160
T = 128
N = 64
PART = F // 8
D = 2048
UNITS = 20
LAST = 16
MESH = pl.DeviceIdType.MESH
BF = jnp.bfloat16
F32 = jnp.float32
ROOT = 1.0 / math.sqrt(2.0)
HBM = pl.BlockSpec(memory_space=pl.ANY)
VMEM = pl.BlockSpec(memory_space=pltpu.VMEM)


OFFSETS = sorted(
    ((a, b, c) for a in range(4) for b in range(4) for c in range(4) if a + b + c),
    key=lambda o: -sum(min(v, 4 - v) for v in o),
)


def dot(left, right, dims=(1, 0)):
    return lax.dot_general(left, right, ((dims[:1], dims[1:]), ((), ())), preferred_element_type=F32)


def halves(a):
    high = a.astype(BF)
    return high, (a - high.astype(F32)).astype(BF)


def dot2(pair, right, dims=(1, 0)):
    return dot(pair[0], right, dims) + dot(pair[1], right, dims)


def dot2r(left, pair, dims=(1, 0)):
    return dot(left, pair[0], dims) + dot(left, pair[1], dims)


def dot3(lefts, rights, dims=(1, 0)):
    return (
        dot(lefts[0], rights[0], dims)
        + dot(lefts[0], rights[1], dims)
        + dot(lefts[1], rights[0], dims)
    )


def ahead(a, d):
    return pltpu.roll(a, (8 - d) % 8, 0) if d % 8 else a


def back(a, d):
    return pltpu.roll(a, d, 0) if d % 8 else a


def phi(u):
    row = lax.broadcasted_iota(jnp.int32, (8, T), 0)
    low, high = u[:8], u[8:]
    tiles = []
    for m, fill in ((low, jnp.zeros((8, T), F32)), (high, (row == 4).astype(F32))):
        tiles.append(m * m * ROOT)
        for d in range(1, 4):
            tiles.append(m * ahead(m, d))
        tiles.append(jnp.where(row < 4, m * ahead(m, 4), fill))
    for d in range(8):
        tiles.append(low * ahead(high, d))
    return jnp.concatenate(tiles + [low, high], 0)


def pull(u, grad):
    row = lax.broadcasted_iota(jnp.int32, (8, T), 0)
    low, high = u[:8], u[8:]
    tile = lambda n: grad[8 * n : 8 * n + 8]
    sums = []
    for at, m in ((0, low), (5, high)):
        total = tile(18 + at // 5) + tile(at) * (2.0 * ROOT) * m
        for d in range(1, 5):
            piece = tile(at + d)
            if d == 4:
                piece = jnp.where(row < 4, piece, 0.0)
            total = total + piece * ahead(m, d) + back(piece * m, d)
        sums.append(total)
    for d in range(8):
        piece = tile(10 + d)
        sums[0] = sums[0] + piece * ahead(high, d)
        sums[1] = sums[1] + back(piece * low, d)
    return jnp.concatenate(sums, 0)


def kernel(
    x_hbm, c_hbm, wq_hbm, wk_hbm, wv_hbm, gi_ref, o_ref,
    x_ref, c_ref, wq_ref, wk_ref, wv_ref,
    uq_ref, uk_ref, fqt, fkt, fqn, fkn, v_ref, ath, atl, ni_ref, rd_ref, gnh, gnl, ga_ref,
    gv_ref, gk_ref, sh_ref, gt_ref,
    s1, s2, s3, s4, t1, t2, t3, t4, nsrc, nrcv, tsrc, trcv,
    xt_ref, xr_ref, xp_ref, gs_ref, gr_ref, gp_ref,
    p_ref, a_ref, b_ref, q_ref, r2_ref, w_ref, r3_ref,
    load, a2s, a2r, lns, lnr, xs, xr, gss, grr, p1s, p1r, p2s, p2r, p4s, p4r, r4_ref, p3s, p3r,
):
    me = lax.axis_index("seq")
    core = lax.axis_index("batch")
    other = 1 - core
    at = (me // 16, (me // 4) % 4, me % 4)
    weight = (16, 4, 1)

    def along(d, c):
        return (me + (c - at[d]) * weight[d], core)

    def copy_to(src, dst, send, recv, device):
        return pltpu.make_async_remote_copy(
            src_ref=src, dst_ref=dst, send_sem=send, recv_sem=recv,
            device_id=device, device_id_type=MESH,
        )

    def push(src, dst, send, recv, device):
        copy = copy_to(src, dst, send, recv, device)
        copy.start()
        return copy

    def drain(ref, sem):
        copy_to(ref, ref, sem, sem, (me, other)).wait_send()

    def peers():
        part = [[(at[d] + k) % 4 * weight[d] for k in range(4)] for d in range(3)]
        return [part[0][a] + part[1][b] + part[2][c] for a, b, c in OFFSETS]

    barrier = pltpu.get_barrier_semaphore()
    for peer in peers():
        pl.semaphore_signal(barrier, inc=1, device_id=(peer, core), device_id_type=MESH)
    pl.semaphore_signal(barrier, inc=1, device_id=(me, other), device_id_type=MESH)

    loads = []
    for n, (src, dst) in enumerate(
        ((x_hbm, x_ref), (wk_hbm, wk_ref), (wq_hbm, wq_ref), (wv_hbm, wv_ref), (c_hbm, c_ref))
    ):
        copy = pltpu.make_async_copy(src, dst, load.at[n])
        copy.start()
        loads.append(copy)

    def scatter(src, dst, n):
        for peer in peers():
            copy_to(src.at[peer], dst.at[me], a2s.at[n], a2r.at[n], (peer, core)).start()
        dst[me] = src[me]

    def arrive_all(dst, n):
        blocks = dst.at[pl.ds(0, N - 1)]
        copy_to(blocks, blocks, a2s.at[n], a2r.at[n], (me, other)).wait_recv()

    def scan(src, dst, n, reverse):
        arrive_all(src, n)

        def step(i, run):
            for k in range(8):
                j = N - 1 - 8 * i - k if reverse else 8 * i + k
                dst[j] = run
                run = run + src[j]
            return run

        lax.fori_loop(0, N // 8, step, jnp.zeros((PART, DV), F32))

    def put_state(dst, h, value):
        for j in range(8):
            dst[8 * h + j, :16, :] = value[16 * j : 16 * j + 16]
            dst[8 * h + j, 16:, :] = value[128 + 4 * j : 132 + 4 * j]

    def get_state(src, h):
        tiles = [src[8 * h + j, :16, :] for j in range(8)]
        tiles += [src[8 * h + j, 16:, :] for j in range(8)]
        return jnp.concatenate(tiles, 0)

    def gather(src, rcv, n):
        for peer in peers():
            copy_to(src, rcv.at[me], lns.at[n], lnr.at[n], (peer, core)).start()
        rcv[me] = src[...]

    def gathered(rcv, n, low, high):
        blocks = rcv.at[pl.ds(0, N - 1)]
        copy_to(blocks, blocks, lns.at[n], lnr.at[n], (me, other)).wait_recv()

        def step(j, total):
            return total + rcv[j]

        total = lax.fori_loop(low, high, step, jnp.zeros((10, DV), F32))
        rows = []
        for h in range(H):
            at_lane = 32 * (h % 4)
            rest = total[8 + h // 4 : 9 + h // 4, at_lane : at_lane + 32]
            rows.append(jnp.concatenate([total[h : h + 1], rest], 1))
        return jnp.concatenate(rows, 0)

    def turn(rows):
        wide = jnp.concatenate([rows, jnp.zeros((8, 256 - F), F32)], 1)
        return jnp.concatenate([wide, jnp.zeros((T - 8, 256), F32)], 0).T[:F]

    causal = lax.broadcasted_iota(jnp.int32, (T, T), 0) >= lax.broadcasted_iota(jnp.int32, (T, T), 1)
    anti = lax.broadcasted_iota(jnp.int32, (T, T), 0) <= lax.broadcasted_iota(jnp.int32, (T, T), 1)
    lane = lax.broadcasted_iota(jnp.int32, (T, DV), 1)
    ones = jnp.ones((T, DV), BF)
    rows8 = lax.broadcasted_iota(jnp.int32, (8, DV), 0)

    loads[0].wait()
    loads[1].wait()
    x = x_ref[...]
    flat = dot(x, wk_ref[...]).T * 0.5
    norm = jnp.zeros((8, DV), F32)
    one = jnp.ones((8, T), BF)
    for h in range(H):
        u = flat[DK * h : DK * h + DK]
        uk_ref[h] = u
        f = phi(u)
        ft = f.astype(BF)
        fkt[h] = ft
        fkn[h] = f.T.astype(BF)
        norm = jnp.where(rows8 == h, dot(one, ft[:DV], (1, 1)), norm)
    nsrc[:8] = norm
    for i in range(2):
        last = jnp.concatenate([fkt[h, DV:] for h in range(4 * i, 4 * i + 4)], 0)
        nsrc[8 + i : 9 + i] = dot(one, last, (1, 1))[:1]
    pl.semaphore_wait(barrier, N)
    gather(nsrc, nrcv, 0)

    loads[3].wait()
    for m in range(4):
        both = dot(x, wv_ref[:, 256 * m : 256 * m + 256]).astype(BF)
        for i in range(2):
            val = both[:, i * DV : (i + 1) * DV]
            v_ref[2 * m + i] = val
            put_state(s1, 2 * m + i, dot(fkt[2 * m + i], val))
    loads[2].wait()
    flat = dot(x, wq_ref[...]).T * 0.5
    for h in range(H):
        u = flat[DK * h : DK * h + DK]
        uq_ref[h] = u
        f = phi(u)
        fqt[h] = f.astype(BF)
        fqn[h] = f.T.astype(BF)

    def inside(h):
        attn = halves(jnp.where(causal, dot(fqn[h], fkt[h]), 0.0))
        both = dot2(attn, jnp.concatenate([v_ref[h], ones], 1))
        ni_ref[h] = both[:, :DV]
        rd_ref[h] = both[:, DV:]
        turned = halves(jnp.where(anti, dot(fkn[h], fqt[h]), 0.0))
        ath[h] = turned[0]
        atl[h] = turned[1]

    for h in range(H):
        inside(h)
    scatter(s1, s2, 0)
    prefix = gathered(nrcv, 0, 0, me)
    loads[4].wait()

    for h in range(H):
        row = halves(jnp.broadcast_to(prefix[h : h + 1], (DV, F)))
        den = rd_ref[h] + dot2r(fqn[h], row, (1, 1))
        scale = 1.0 / den
        rd_ref[h] = scale
        numer = c_ref[:, h * DV : (h + 1) * DV].astype(F32) * scale
        gn = halves(numer)
        gnh[h] = gn[0]
        gnl[h] = gn[1]
        put_state(t1, h, dot2r(fqt[h], gn))
    scatter(t1, t2, 2)

    for h in range(H):
        gn = (gnh[h], gnl[h])
        gv_ref[h] = dot3((ath[h], atl[h]), gn)
        ga_ref[h] = dot2(gn, v_ref[h], (1, 1))

    scan(s2, s3, 0, False)
    scatter(s3, s4, 1)

    for b in range(D // 128):
        block = x_ref[:, b * 128 : (b + 1) * 128].astype(F32).T
        for i in range(4):
            for half in range(2):
                row = 32 * i + 16 * half
                xt_ref[half, 4 * b + i] = block[row : row + 16]
    swap = push(xt_ref.at[other], xr_ref, xs.at[0], xr.at[0], (me, other))
    xp_ref[:, :T] = xt_ref[core].reshape(D // 2, T).astype(BF)

    scan(t2, t3, 2, True)
    scatter(t3, t4, 3)

    def share(m, value):
        gp_ref[:T, 256 * m : 256 * m + 256] = value
        gs_ref[m] = value.astype(F32)
        return push(gs_ref.at[m], gr_ref.at[m], gss.at[0], grr.at[m], (me, other))

    turned = turn(prefix)
    columns = halves(turned)
    arrive_all(s4, 1)
    down = jnp.zeros((F, DV), F32)
    grads = []
    for h in range(H):
        state = halves(get_state(s4, h))
        gn = (gnh[h], gnl[h])
        num = ni_ref[h] + dot2r(fqn[h], state)
        numer = gn[0].astype(F32) + gn[1].astype(F32)
        denom = -jnp.sum(numer * num, 1, keepdims=True) * rd_ref[h]
        ga = halves(jnp.where(causal, ga_ref[h] + denom, 0.0))
        mine = halves(jnp.where(lane == h, denom, 0.0))
        left = [jnp.concatenate([s, c], 1) for s, c in zip(state, columns)]
        right = [jnp.concatenate([g, m], 1) for g, m in zip(gn, mine)]
        gfq = dot2r(fkt[h], ga, (1, 1)) + dot3(left, right, (1, 1))
        grads.append(pull(uq_ref[h], gfq) * 0.5)
        gk_ref[h] = dot2r(fqt[h], ga)
        down = down + dot2r(fqt[h], mine)
    rows = jnp.concatenate([down, jnp.zeros((256 - F, DV), F32)], 0).T
    tsrc[:8] = rows[:8, :DV]
    for i in range(2):
        tsrc[8 + i : 9 + i] = jnp.concatenate(
            [rows[h : h + 1, DV:F] for h in range(4 * i, 4 * i + 4)], 1
        )
    gather(tsrc, trcv, 1)
    grad_q = jnp.concatenate(grads, 0).T.astype(BF)

    arrive_all(t4, 3)
    shares = []
    for m in range(4):
        pieces = []
        for h in (2 * m, 2 * m + 1):
            state = halves(get_state(t4, h))
            sh_ref[h] = state[0]
            gt_ref[h] = state[1]
            pieces.append((gv_ref[h] + dot2r(fkn[h], state)).astype(BF))
        shares.append(share(m, jnp.concatenate(pieces, 1)))

    swap.wait_recv()
    xp_ref[:, T:] = xr_ref[...].reshape(D // 2, T).astype(BF)

    def multiply(m):
        shares[m].wait_recv()
        gp_ref[T:, 256 * m : 256 * m + 256] = gr_ref[m].astype(BF)
        right = gp_ref[:, 256 * m : 256 * m + 256]
        for z in range(4):
            part = dot(xp_ref[256 * z : 256 * z + 256, :], right)
            for i in range(2):
                block = part[:, i * DV : (i + 1) * DV].reshape(4, 4, 2, 8, DV)
                for r in range(2):
                    p_ref[4 * m + 2 * i + r, z] = block[:, :, r]

    def line_part(u, g, c, half):
        take = pl.ds(2 * half, 2)
        if g == 0:
            return (u, c, take)
        if g == 1:
            return (u, take, c)
        return (u, take, slice(None), c)

    def arrived(ref, sem, u, more=()):
        if u % 2 == 0:
            pair = ref.at[(pl.ds(u, 2),) + more]
            copy_to(pair, pair, sem, sem, (me, other)).wait_recv()

    def stage0(u):
        g = u % 3
        i = at[g]
        right, left, far = (i + 1) % 4, (i + 3) % 4, (i + 2) % 4
        keys = (
            (far, 0, right, a_ref.at[u, 0]),
            (far, 1, left, a_ref.at[u, 1]),
            (right, 1, right, b_ref.at[u, 0, pl.ds(2, 2)]),
            (left, 0, left, b_ref.at[u, 1, pl.ds(0, 2)]),
        )
        for n, (c, half, peer, dst) in enumerate(keys):
            push(p_ref.at[line_part(u, g, c, half)], dst, p1s.at[0], p1r.at[u // 2, n // 2], along(g, peer))

    def stage1(u):
        g = u % 3
        i = at[g]
        right, left = (i + 1) % 4, (i + 3) % 4
        arrived(a_ref, p1r.at[u // 2, 0], u)
        for n, (peer, half) in enumerate(((right, 0), (left, 1))):
            where = line_part(u, g, peer, half)
            p_ref[where] = p_ref[where] + a_ref[u, n]
            dst = b_ref.at[u, n, pl.ds(2 * half, 2)]
            push(p_ref.at[where], dst, p1s.at[1], p1r.at[u // 2, 1], along(g, peer))

    order = ((1, 2), (2, 0), (0, 1))

    def stage2(u):
        g = u % 3
        arrived(b_ref, p1r.at[u // 2, 1], u)
        for half in range(2):
            mine = p_ref[line_part(u, g, at[g], half)]
            mine = mine + b_ref[u, 0, 2 * half : 2 * half + 2] + b_ref[u, 1, 2 * half : 2 * half + 2]
            for i in range(2):
                if g == 1:
                    q_ref[u, :, 2 * half + i] = mine[i]
                else:
                    q_ref[u, 2 * half + i] = mine[i]
        d, e = order[g]
        if u >= LAST:
            for k in range(1, 16):
                a, b = (at[d] + k // 4) % 4, (at[e] + k % 4) % 4
                peer = me + (a - at[d]) * weight[d] + (b - at[e]) * weight[e]
                dst = r4_ref.at[u - LAST, 4 * at[d] + at[e]]
                push(q_ref.at[u, a, b], dst, p4s.at[0], p4r.at[u // 2 - LAST // 2], (peer, core))
            return
        for k in range(1, 4):
            c = (at[d] + k) % 4
            push(q_ref.at[u, c], r2_ref.at[u, at[d]], p2s.at[0], p2r.at[u // 2], along(d, c))

    def from_line(d, src, dst, recv, u):
        arrived(dst, recv.at[u // 2], u, (pl.ds(0, 3),))
        total = src[u, at[d]]
        for k in range(1, 4):
            total = total + dst[u, (at[d] + k) % 4]
        return total

    def stage3(u):
        if u >= LAST:
            return
        d, e = order[u % 3]
        w_ref[u] = from_line(d, q_ref, r2_ref, p2r, u)
        for k in range(1, 4):
            c = (at[e] + k) % 4
            push(w_ref.at[u, c], r3_ref.at[u, at[e]], p3s.at[0], p3r.at[u // 2], along(e, c))

    def stage4(u):
        if u < LAST:
            total = from_line(order[u % 3][1], w_ref, r3_ref, p3r, u)
        else:
            n = u - LAST
            arrived(r4_ref, p4r.at[n // 2], n, (pl.ds(0, 15),))
            d, e = order[u % 3]
            r4_ref[n, 4 * at[d] + at[e]] = q_ref[u, at[d], at[e]]
            total = r4_ref[n, 0]
            for k in range(1, 16):
                total = total + r4_ref[n, k]
        piece, r = u // 2, u % 2
        rows = slice(8 * r, 8 * r + 8)
        o_ref[rows, piece * DV : (piece + 1) * DV] = total

    for m in range(4):
        multiply(m)
        for u in range(4 * m, 4 * m + 4):
            stage0(u)
    for u in range(4):
        stage1(u)
    suffix = gathered(trcv, 1, me + 1, N)
    turned = turn(suffix)
    grads = []
    for h in range(H):
        gfk = gk_ref[h] + dot2((sh_ref[h], gt_ref[h]), v_ref[h], (1, 1)) + turned[:, h : h + 1]
        grads.append(pull(uk_ref[h], gfk) * 0.5)
    grad_k = jnp.concatenate(grads, 0).T.astype(BF)
    shares.append(share(4, jnp.concatenate([grad_q, grad_k], 1)))
    for m in range(4, 5):
        multiply(m)
        for u in range(4 * m, 4 * m + 4):
            stage0(u)
    wide = D // 8

    def inputs(n):
        cut = slice(n * wide, (n + 1) * wide)
        total = dot(gp_ref[:T, : H * DV], wv_ref[cut, :], (1, 1))
        total = total + dot(gp_ref[:T, H * DV : H * DV + 128], wq_ref[cut, :], (1, 1))
        total = total + dot(gp_ref[:T, H * DV + 128 :], wk_ref[cut, :], (1, 1))
        gi_ref[:, cut] = total.astype(BF)

    for n in range(4):
        inputs(n)
    for u in range(4, 8):
        stage1(u)
    for n in range(4, 8):
        inputs(n)
    for u in range(8, 20):
        stage1(u)
        if u >= 14:
            stage2(u - 14)
    for u in range(6, 20):
        stage2(u)
        if u >= 12:
            stage3(u - 12)
    for u in range(8, 20):
        stage3(u)
        if u >= 14:
            stage4(u - 14)
    for u in range(6, 20):
        stage4(u)
    for n, src in enumerate((s1, s3, t1, t3)):
        drain(src.at[pl.ds(0, N - 1)], a2s.at[n])
    for n, rcv in enumerate((nrcv, trcv)):
        drain(rcv.at[pl.ds(0, N - 1)], lns.at[n])
    drain(xr_ref, xs.at[0])
    drain(gr_ref, gss.at[0])
    drain(b_ref, p1s.at[0])
    drain(a_ref, p1s.at[1])
    drain(q_ref.at[pl.ds(0, LAST), pl.ds(0, 3)], p2s.at[0])
    drain(w_ref.at[pl.ds(0, LAST), pl.ds(0, 3)], p3s.at[0])
    drain(r4_ref.at[:, pl.ds(0, 15)], p4s.at[0])


def results(g_ref, w_ref, gi_ref, oq_ref, ok_ref, ov_ref, save):
    writes = [
        pltpu.make_async_copy(g_ref, gi_ref, save.at[0]),
        pltpu.make_async_copy(w_ref.at[:, pl.ds(0, H * DV)], ov_ref, save.at[1]),
        pltpu.make_async_copy(w_ref.at[:, pl.ds(H * DV, 128)], oq_ref, save.at[2]),
        pltpu.make_async_copy(w_ref.at[:, pl.ds(H * DV + 128, 128)], ok_ref, save.at[3]),
    ]
    for copy in writes:
        copy.start()
    for copy in writes:
        copy.wait()


def body(inputs, cotangent, w_query, w_key, w_value):
    vm = lambda *shape: pltpu.VMEM(shape, F32)
    vb = lambda *shape: pltpu.VMEM(shape, BF)
    sems = lambda *sizes: pltpu.SemaphoreType.DMA(sizes)
    state = lambda: vm(N, PART, DV)
    scratch = [
        vb(T, D), vb(T, H * DV), vb(D, 128), vb(D, 128), vb(D, H * DV),
        vm(H, DK, T), vm(H, DK, T), vb(H, F, T), vb(H, F, T), vb(H, T, F), vb(H, T, F), vb(H, T, DV),
        vb(H, T, T), vb(H, T, T), vm(H, T, DV), vm(H, T, DV), vb(H, T, DV), vb(H, T, DV), vm(H, T, T),
        vm(H, T, DV), vm(H, F, T), vb(H, F, DV), vb(H, F, DV),
        state(), state(), state(), state(), state(), state(), state(), state(),
        vm(10, DV), vm(N, 10, DV), vm(10, DV), vm(N, 10, DV),
        vm(2, N, 16, T), vm(N, 16, T), vb(D // 2, 2 * T), vm(5, T, 256), vm(5, T, 256), vb(2 * T, 1280),
        vm(UNITS, 4, 4, 4, 8, DV), vm(UNITS, 2, 2, 4, 8, DV), vm(UNITS, 2, 4, 4, 8, DV),
        vm(UNITS, 4, 4, 8, DV), vm(UNITS, 4, 4, 8, DV), vm(UNITS, 4, 8, DV), vm(UNITS, 4, 8, DV),
        sems(5), sems(4), sems(4), sems(2), sems(2), sems(1), sems(1), sems(1), sems(5),
        sems(2), sems(UNITS // 2, 2), sems(1), sems(UNITS // 2), sems(1), sems(2), vm(UNITS - LAST, 16, 8, DV), sems(1), sems(UNITS // 2),
    ]
    grad_in, grad_w = pl.pallas_call(
        kernel,
        out_shape=[vb(T, D), vm(16, 1280)],
        in_specs=[HBM] * 5,
        out_specs=[VMEM] * 2,
        scratch_shapes=scratch,
        compiler_params=pltpu.CompilerParams(
            collective_id=0, has_side_effects=True, vmem_limit_bytes=60 << 20
        ),
    )(inputs[0], cotangent[0], w_query, w_key, w_value)
    grad_in, grad_wq, grad_wk, grad_wv = pl.pallas_call(
        results,
        out_shape=[
            jax.ShapeDtypeStruct((T, D), BF),
            jax.ShapeDtypeStruct((16, 128), F32),
            jax.ShapeDtypeStruct((16, 128), F32),
            jax.ShapeDtypeStruct((16, H * DV), F32),
        ],
        in_specs=[VMEM] * 2,
        out_specs=[HBM] * 4,
        scratch_shapes=[sems(4)],
    )(*(pltpu.with_memory_space_constraint(g, pltpu.VMEM) for g in (grad_in, grad_w)))
    return (grad_in[None], grad_wq, grad_wk, grad_wv)


def solution(mesh):
    in_specs = (P("batch", "seq", None), P("batch", "seq", None), P(), P(), P())
    out_specs = (
        P("batch", "seq", None),
        P(("seq", "batch"), None),
        P(("seq", "batch"), None),
        P(("seq", "batch"), None),
    )
    return jax.shard_map(body, mesh=mesh, in_specs=in_specs, out_specs=out_specs, check_vma=False)
```
